32 devices in a mesh: cube: 2 (over y), gz: 8 (over z, x), gy: 2 (over core).
Axes of the slice: x: 2, y: 2, z: 4, core: 2. Of those that a mesh axis runs over, the one named last changes fastest.
Arguments:
- noisy_cube: float32 [64, 64, 256], P(('cube', 'gz'), 'gy'), parts along dimension 0, may hold values from -40 to 40
- thresholds: float32 [4], replicated, may hold values from 0.5 to 4
Outputs:
- denoised: float32 [64, 4, 64, 256], P(('cube', 'gz'), None, 'gy'), parts along dimension 0
- gcv_score: float32 [8], P('cube'), parts along dimension 0
The draws below stay inside these ranges and needn't reach their ends.
There are 2 independent parts, one for each index of `cube`. The reference program is written for one: setup_inputs(seed, part) draws one part's arguments, and reference() takes and returns one part's arrays. A program takes and returns all parts, laid end to end along the dimension named above; an argument that names none is the same for every part. Nothing has to cross between parts.
All inputs are finite; a program needn't handle non-finite values.
Results may differ from the reference program's by a relative error of at most 0.0003.
Values sent between devices are 32-bit elements; how exact they have to be, the bound alone decides.
No kernel may reach another device: no remote copies, remote signals or barrier semaphores. Data moves between devices by JAX's collectives and lax.ppermute only.
A program may use at most 64 MiB of HBM per device.

```python
import math
import jax
import jax.numpy as jnp
from jax import lax

NX = 256
NT = 4
NZ = 32
NY = 64


def draw_noisy_cube(key, part):
    subkeys = jax.random.split(jax.random.fold_in(key, 17), 2)
    phases = jax.random.uniform(subkeys[0], (3,), jnp.float32, -math.pi, math.pi)
    z_frac = jnp.arange(NZ, dtype=jnp.float32) / NZ
    y_frac = jnp.arange(NY, dtype=jnp.float32) / NY
    x_frac = jnp.arange(NX, dtype=jnp.float32) / NX
    signal = 2.0 * jnp.sin(2.0 * math.pi * 3.0 * z_frac + phases[0])[:, None, None]
    signal = signal * jnp.cos(2.0 * math.pi * 2.0 * y_frac + phases[1])[None, :, None]
    signal = signal * jnp.sin(2.0 * math.pi * 5.0 * x_frac + phases[2])[None, None, :]
    z_rise = 3.0 ** (jnp.arange(NZ, dtype=jnp.float32) / (NZ - 1))
    y_rise = 3.0 ** (jnp.arange(NY, dtype=jnp.float32) / (NY - 1))
    scaling = z_rise[:, None, None] * y_rise[None, :, None]
    jitter = jax.random.truncated_normal(subkeys[1], -4.0, 4.0, (NZ, NY, NX), jnp.float32)
    return signal + scaling * jitter


def setup_inputs(seed: int = 0, part: int = 0) -> dict:
    arg_keys = jax.random.split(jax.random.key(seed), 3)
    part_keys = jax.random.split(jax.random.fold_in(arg_keys[2], part), 3)
    return {
        "noisy_cube": draw_noisy_cube(jax.random.fold_in(jax.random.fold_in(arg_keys[2], part), 71), part),
        "thresholds": jnp.clip(jnp.exp(jax.random.uniform(arg_keys[1], (NT,), jnp.float32, math.log(0.5), math.log(4.0))), 0.5, 4.0),
    }


LOWPASS = (0.2303778133088964, 0.7148465705529154, 0.6308807679298587, -0.0279837694168599,
           -0.1870348117190931, 0.0308413818355607, 0.0328830116668852, -0.0105974017850690)
HIGHPASS = tuple(((-1) ** tap_index) * LOWPASS[7 - tap_index] for tap_index in range(8))
lead_taps = 6
trail_taps = 3


def analyse(extended, dimension_number, axis_length):
    lowband = 0.0
    highband = 0.0
    for tap_index in range(8):
        sliced = lax.slice_in_dim(extended, tap_index, tap_index + axis_length - 1, 2, dimension_number)
        lowband = lowband + LOWPASS[tap_index] * sliced
        highband = highband + HIGHPASS[tap_index] * sliced
    return lowband, highband


def synthesise(lowband, highband, dimension_number, axis_length):
    even_part = 0.0
    odd_part = 0.0
    for tap_index in range(4):
        low_slice = lax.slice_in_dim(lowband, 3 - tap_index, 3 - tap_index + axis_length, 1, dimension_number)
        high_slice = lax.slice_in_dim(highband, 3 - tap_index, 3 - tap_index + axis_length, 1, dimension_number)
        even_part = even_part + LOWPASS[2 * tap_index] * low_slice + HIGHPASS[2 * tap_index] * high_slice
        odd_part = odd_part + LOWPASS[2 * tap_index + 1] * low_slice + HIGHPASS[2 * tap_index + 1] * high_slice
    paired = jnp.stack([even_part, odd_part], dimension_number + 1)
    target = list(even_part.shape)
    target[dimension_number] = 2 * axis_length
    return paired.reshape(target)


def merge_bands(lowband, highband):
    stacked = jnp.stack([lowband, highband], 2)
    return stacked.reshape((lowband.shape[0], 2 * lowband.shape[1]) + lowband.shape[2:])


def split_bands(current):
    halves = current.reshape((current.shape[0], current.shape[1] // 2, 2) + current.shape[2:])
    return halves[:, :, 0], halves[:, :, 1]


def wrap_ahead(input_tensor, dimension_number, border_extent):
    return jnp.concatenate([input_tensor, lax.slice_in_dim(input_tensor, 0, border_extent, 1, dimension_number)], dimension_number)


def wrap_behind(input_tensor, dimension_number, border_extent):
    axis_length = input_tensor.shape[dimension_number]
    return jnp.concatenate([lax.slice_in_dim(input_tensor, axis_length - border_extent, axis_length, 1, dimension_number), input_tensor], dimension_number)


def forward_level(volume):
    planes, number_of_lines, col_count = volume.shape[0], volume.shape[2], volume.shape[3]
    lowband, highband = analyse(wrap_ahead(volume, 0, lead_taps), 0, planes)
    banded = merge_bands(lowband, highband)
    lowband, highband = analyse(wrap_ahead(banded, 2, lead_taps), 2, number_of_lines)
    banded = merge_bands(lowband, highband)
    lowband, highband = analyse(wrap_ahead(banded, 3, lead_taps), 3, col_count)
    return merge_bands(lowband, highband)


def synth_x(current):
    lowband, highband = split_bands(current)
    return synthesise(wrap_behind(lowband, 3, trail_taps), wrap_behind(highband, 3, trail_taps), 3, current.shape[3])


def synth_y(extended, number_of_lines):
    lowband, highband = split_bands(extended)
    return synthesise(lowband, highband, 2, number_of_lines)


def synth_z(extended, planes):
    lowband, highband = split_bands(extended)
    return synthesise(lowband, highband, 0, planes)


def inverse_level(coeffs):
    planes, number_of_lines = coeffs.shape[0], coeffs.shape[2]
    current = synth_x(coeffs)
    current = synth_y(wrap_behind(current, 2, trail_taps), number_of_lines)
    return synth_z(wrap_behind(current, 0, trail_taps), planes)


def spread(details, approximation, limits):
    bounds = limits[None, :, None, None, None]
    widened = details[:, None]
    shrunk = widened - jnp.clip(widened, -bounds, bounds)
    complete = jnp.concatenate([approximation[:, :, None], shrunk], 2)
    return complete.reshape((complete.shape[0], complete.shape[1] * 8) + complete.shape[3:])


def reference(noisy_cube, thresholds):
    level_one = forward_level(noisy_cube[:, None])
    level_two = forward_level(level_one[:, :1])
    details_one = level_one[:, 1:]
    details_two = level_two[:, 1:]
    cell_count = NZ * NY * NX

    def single(threshold):
        limits = threshold[None]
        approximation = inverse_level(spread(details_two, level_two[:, :1], limits))
        rebuilt = inverse_level(spread(details_one, approximation, limits))[:, 0]
        residual = jnp.sum((rebuilt - noisy_cube) ** 2)
        square = threshold * threshold
        zero_weight = jnp.sum(square / (square + details_one * details_one)) + jnp.sum(square / (square + details_two * details_two))
        return rebuilt, cell_count * residual / (zero_weight * zero_weight)

    stacked, gcv_score = lax.map(single, thresholds)
    return jnp.transpose(stacked, (1, 0, 2, 3)), gcv_score
```

```python
import functools
import numpy as np
import jax
import jax.numpy as jnp
from jax import lax
from jax.experimental import pallas as pl
from jax.experimental.pallas import tpu as pltpu
from jax.sharding import PartitionSpec as P

LOWPASS = (
    0.2303778133088964,
    0.7148465705529155,
    0.6308807679298587,
    -0.0279837694168599,
    -0.1870348117190931,
    0.0308413818355607,
    0.0328830116668852,
    -0.010597401785069,
)
HIGHPASS = tuple((-1) ** tap * LOWPASS[7 - tap] for tap in range(8))
FILTERS = (LOWPASS, HIGHPASS)


def analysis_matrix(length):
    half = length // 2
    matrix = np.zeros((length, length))
    for band in range(2):
        for k in range(half):
            for tap in range(8):
                matrix[band * half + k, (2 * k + tap) % length] += FILTERS[band][tap]
    return matrix


def row_order(own_rows, halo):
    lo = list(range(own_rows))
    before = list(range(-halo, 0))
    return lo, before


def dot(a, b):
    return lax.dot_general(
        a, b, (((1,), (0,)), ((), ())),
        precision=lax.Precision.HIGHEST, preferred_element_type=jnp.float32,
    )


def weighted(terms):
    total = None
    for weight, value in terms:
        part = value * weight
        total = part if total is None else total + part
    return total


def plane_kernel(own_ref, other_ref, y_ref, x_ref, out_ref, head_ref, scratch):
    planes, rows, _ = own_ref.shape
    out_rows = out_ref.shape[1]
    for z in range(planes):
        plane = jnp.concatenate([own_ref[z], other_ref[z]], 0)
        scratch[pl.ds(z * out_rows, out_rows), :] = dot(y_ref[...], plane)
    result = dot(scratch[...], x_ref[...])
    for z in range(planes):
        out_ref[z] = result[z * out_rows : (z + 1) * out_rows]
    for z in range(head_ref.shape[0]):
        head_ref[z] = result[z * out_rows : (z + 1) * out_rows]


def tally(value, limit_squares, sums, keep=None):
    square = value * value
    for t, limit in enumerate(limit_squares):
        weight = 1.0 / (square + limit)
        cut = jnp.minimum(square, limit)
        if keep is not None:
            weight = jnp.where(keep, weight, 0.0)
            cut = jnp.where(keep, cut, 0.0)
        sums[0][t] = weight if sums[0][t] is None else sums[0][t] + weight
        sums[1][t] = cut if sums[1][t] is None else sums[1][t] + cut


def fold(sums):
    rows = [jnp.sum(a, axis=0, keepdims=True) for group in sums for a in group]
    return jnp.concatenate(rows, 0)


def depth_kernel(limits_ref, own_ref, next_ref, after_ref, out_ref, tail_ref, parcel_ref):
    planes, rows, cols = own_ref.shape
    own_lo = parcel_ref.shape[0] // 8 * 8
    limits = [limits_ref[t] for t in range(limits_ref.shape[0])]
    squares = [t * t for t in limits]
    half_cols = cols // 2
    lo_rows = (parcel_ref.shape[0] - 2 * len(limits)) // (planes // 2)
    sums = [[None] * len(limits), [None] * len(limits)]

    def source(i, r, c):
        at = (pl.ds(r, 8), pl.ds(c, half_cols))
        if i < planes:
            return own_ref[(i,) + at]
        if i < 2 * planes:
            return next_ref[(i - planes,) + at]
        return after_ref[(i - 2 * planes,) + at]

    for r in range(0, rows, 8):
        for c in range(0, cols, half_cols):
            tile = [source(i, r, c) for i in range(planes + 6)]
            for k in range(planes // 2):
                for band in range(2):
                    value = weighted((FILTERS[band][tap], tile[2 * k + tap]) for tap in range(8))
                    out_ref[2 * k + band, pl.ds(r, 8), pl.ds(c, half_cols)] = value
                    if k == planes // 2 - 1:
                        tail_ref[band, pl.ds(r, 8), pl.ds(c, half_cols)] = value
                    if r < 2 * lo_rows:
                        if band == 0 and c == 0 and r < lo_rows:
                            parcel_ref[pl.ds(k * lo_rows + r, 8), :] = value
                        else:
                            tally(value, squares, sums)
    parcel_ref[pl.ds(planes // 2 * lo_rows, 2 * len(limits)), :] = fold(sums)


def final_kernel(
    full, cells, index_ref, limits_ref, parcels_ref, own_ref, before_ref, tail_ref,
    ya_ref, xa_ref, ysa_ref, xsa_ref, ys_ref, xs_ref,
    out_ref, score_ref, zed, mix, coarse_in, coarse_mid, coarse, wide, wide_y,
):
    planes, rows, cols = own_ref.shape
    count = limits_ref.shape[0]
    half_cols = cols // 2
    limits = [limits_ref[t] for t in range(count)]
    squares = [t * t for t in limits]
    lo_rows = (parcels_ref.shape[2] - 2 * count) // (planes // 2)
    deep_rows = 2 * lo_rows
    pieces = parcels_ref.shape[1]
    depth = planes // 2
    kappas = list(range(-5, -5 + pieces)) if full else list(range(-5, 1))

    def coarse_plane(r, side, i):
        if full:
            r = r % (depth * pieces)
        at = index_ref[r // depth]
        return parcels_ref[side, at, pl.ds((r % depth) * lo_rows + i, 8), :]

    for side in range(2):
        for i in range(0, lo_rows, 8):
            needed = sorted({(2 * kap + 10 + tap) % (depth * pieces) if full else 2 * kap + 10 + tap
                             for kap in kappas for tap in range(8)})
            tile = {r: coarse_plane(r, side, i) for r in needed}
            for a, kap in enumerate(kappas):
                for band in range(2):
                    terms = []
                    for tap in range(8):
                        r = 2 * kap + 10 + tap
                        terms.append((FILTERS[band][tap], tile[r % (depth * pieces) if full else r]))
                    zed[2 * a + band, pl.ds(side * lo_rows + i, 8), :] = weighted(terms)
    for a in range(2 * len(kappas)):
        mix[pl.ds(a * deep_rows, deep_rows), :] = dot(ya_ref[...], zed[a])
    mix[...] = dot(mix[...], xa_ref[...])

    low_lanes = lax.broadcasted_iota(jnp.int32, (8, half_cols), 1) < half_cols // 2
    sums = [[None] * count, [None] * count]
    for a, kap in enumerate(kappas):
        if not full and kap != 0:
            continue
        for band in range(2):
            for i in range(0, deep_rows, 8):
                if not full and i % lo_rows >= lo_rows // 2:
                    continue
                kept = band == 0 and i < lo_rows
                value = mix[pl.ds((2 * a + band) * deep_rows + i, 8), :]
                tally(value, squares, sums, ~low_lanes if kept else None)
    total = fold(sums)
    if full:
        for side in range(2):
            for piece in range(pieces):
                total = total + parcels_ref[side, piece, pl.ds(depth * lo_rows, 2 * count), :]
    else:
        total = total + parcels_ref[0, index_ref[5], pl.ds(depth * lo_rows, 2 * count), :]
    for t in range(count):
        weight = jnp.sum(total[t : t + 1]) * squares[t]
        residual = jnp.sum(total[count + t : count + t + 1])
        if full:
            score_ref[t] = cells * residual / (weight * weight)
        else:
            score_ref[t] = weight
            score_ref[count + t] = residual

    back = [(-2, 1), (-1, 0), (-1, 1), (0, 0), (0, 1)]
    for t in range(count):
        for i in range(0, deep_rows, 8):
            shrunk = {}
            for a, kap in enumerate(kappas):
                if kap > 0:
                    continue
                for band in range(2):
                    value = mix[pl.ds((2 * a + band) * deep_rows + i, 8), :]
                    cut = value - jnp.clip(value, -limits[t], limits[t])
                    if band == 0 and i < lo_rows:
                        cut = jnp.where(low_lanes, value, cut)
                    shrunk[kap, band] = cut
            for b, (p, odd) in enumerate(back):
                coarse_in[t * 5 + b, pl.ds(i, 8), :] = weighted(
                    (FILTERS[band][2 * j + odd], shrunk[p - j, band])
                    for j in range(4) for band in range(2)
                )
    halo_rows = coarse.shape[1]
    for s in range(5 * count):
        coarse_mid[pl.ds(s * halo_rows, halo_rows), :] = dot(ysa_ref[...], coarse_in[s])
    spread = dot(coarse_mid[...], xsa_ref[...])
    for s in range(5 * count):
        coarse[s] = spread[s * halo_rows : (s + 1) * halo_rows]

    def source(kap, band, r, c):
        at = (pl.ds(r, 8), pl.ds(c, half_cols))
        if kap == -3:
            return tail_ref[(band,) + at]
        if kap < 0:
            return before_ref[(2 * (kap + 2) + band,) + at]
        return own_ref[(2 * kap + band,) + at]

    first = lax.broadcasted_iota(jnp.int32, (8, half_cols), 0) < 4
    for r in range(0, rows, 8):
        for c in range(0, cols, half_cols):
            for t in range(count):
                shrunk = {}
                for kap in range(-3, 2):
                    for band in range(2):
                        value = source(kap, band, r, c)
                        cut = value - jnp.clip(value, -limits[t], limits[t])
                        if band == 0 and c == 0:
                            if r < lo_rows:
                                cut = coarse[t * 5 + kap + 3, pl.ds(r, 8), :]
                            elif r >= 2 * lo_rows:
                                low = coarse[t * 5 + kap + 3, pl.ds(lo_rows, 8), :]
                                cut = jnp.where(first, low, cut)
                        shrunk[kap, band] = cut
                for z in range(planes):
                    wide[t * planes + z, pl.ds(r, 8), pl.ds(c, half_cols)] = weighted(
                        (FILTERS[band][2 * j + z % 2], shrunk[z // 2 - j, band])
                        for j in range(4) for band in range(2)
                    )
    y_rows = ys_ref.shape[0]
    for s in range(count * planes):
        wide_y[pl.ds(s * y_rows, y_rows), :] = dot(ys_ref[...], wide[s])
    result = dot(wide_y[...], xs_ref[...])
    for t in range(count):
        for z in range(planes):
            s = t * planes + z
            out_ref[z, t] = result[s * y_rows : (s + 1) * y_rows]


def shifted(array, axis, by):
    devices = lax.axis_size(axis)
    return lax.ppermute(array, axis, [(i, (i + by) % devices) for i in range(devices)])


VMEM = pl.BlockSpec(memory_space=pltpu.VMEM)
SMEM = pl.BlockSpec(memory_space=pltpu.SMEM)
PARAMS = pltpu.CompilerParams(vmem_limit_bytes=24 * 1024 * 1024)


def struct(*shape):
    return jax.ShapeDtypeStruct(shape, jnp.float32)


def constant(matrix):
    return jnp.asarray(np.ascontiguousarray(matrix), jnp.float32)


def body(noisy_cube, thresholds):
    planes, rows, cols = noisy_cube.shape
    count = thresholds.shape[0]
    n = lax.axis_size("gz")
    if lax.axis_size("gy") != 2 or planes != 4:
        raise ValueError("unsupported split")
    lo_rows = rows // 2
    pad = 4
    all_rows = 2 * lo_rows + 2 * pad
    full = n <= 8

    y_all = analysis_matrix(2 * rows)
    y_matrix = np.zeros((all_rows, 2 * rows))
    y_matrix[:lo_rows] = y_all[:lo_rows]
    y_matrix[lo_rows : 2 * lo_rows] = y_all[rows : rows + lo_rows]
    for band in range(2):
        start = 2 * lo_rows + band * pad
        stop = (band + 1) * rows
        y_matrix[start : start + 3] = y_all[stop - 3 : stop]
    x_matrix = analysis_matrix(cols)
    deep = analysis_matrix(rows)
    deep_x = analysis_matrix(cols // 2)
    picked = np.zeros((lo_rows + 8, rows))
    picked[:lo_rows] = deep[:, :lo_rows].T
    picked[lo_rows : lo_rows + 3] = deep[:, rows - 3 :].T

    other = shifted(noisy_cube, "gy", 1)
    flat, head = pl.pallas_call(
        plane_kernel,
        out_shape=(struct(planes, all_rows, cols), struct(2, all_rows, cols)),
        in_specs=[VMEM] * 4,
        out_specs=(VMEM, VMEM),
        scratch_shapes=[pltpu.VMEM((planes * all_rows, cols), jnp.float32)],
        compiler_params=PARAMS,
        name="plane",
    )(noisy_cube, other, constant(y_matrix), constant(x_matrix.T))

    after_one = shifted(flat, "gz", -1)
    after_two = shifted(head, "gz", -2)
    own, tail, parcel = pl.pallas_call(
        depth_kernel,
        out_shape=(
            struct(planes, all_rows, cols),
            struct(2, all_rows, cols),
            struct(planes // 2 * lo_rows + 2 * count, cols // 2),
        ),
        in_specs=[SMEM] + [VMEM] * 3,
        out_specs=(VMEM,) * 3,
        compiler_params=PARAMS,
        name="depth",
    )(thresholds, flat, after_one, after_two)

    place = lax.axis_index("gz")
    offsets = jnp.arange(-5, 4)
    if full:
        pairs = n // 2
        column = jnp.stack([parcel] + [shifted(parcel, "gz", -2 * q) for q in range(1, pairs)])
        swapped = lax.ppermute(column, "gz", [(i, i ^ 1) for i in range(n)])
        side = jnp.concatenate([column, swapped])
        inside = place % 2
        spot = (inside + offsets) % n
        index = ((spot % 2) ^ inside) * pairs + spot // 2
    else:
        side = jnp.stack([parcel if o == 0 else shifted(parcel, "gz", -o) for o in range(-5, 4)])
        index = offsets + 5
    parcels = jnp.stack([side, shifted(side, "gy", 1)])
    before = shifted(own, "gz", 1)
    before_two = shifted(tail, "gz", 2)

    kappas = n if full else 6
    y_rows = rows
    cells = float(planes * rows * cols * n * 2)
    denoised, score = pl.pallas_call(
        functools.partial(final_kernel, full, cells),
        out_shape=(
            struct(planes, count, rows, cols),
            struct(count if full else 2 * count),
        ),
        in_specs=[SMEM] * 2 + [VMEM] * 10,
        out_specs=(VMEM, SMEM),
        scratch_shapes=[
            pltpu.VMEM((2 * kappas, rows, cols // 2), jnp.float32),
            pltpu.VMEM((2 * kappas * rows, cols // 2), jnp.float32),
            pltpu.VMEM((5 * count, rows, cols // 2), jnp.float32),
            pltpu.VMEM((5 * count * (lo_rows + 8), cols // 2), jnp.float32),
            pltpu.VMEM((5 * count, lo_rows + 8, cols // 2), jnp.float32),
            pltpu.VMEM((count * planes, all_rows, cols), jnp.float32),
            pltpu.VMEM((count * planes * rows, cols), jnp.float32),
        ],
        compiler_params=PARAMS,
        name="final",
    )(
        index.astype(jnp.int32), thresholds, parcels, own, before, before_two,
        constant(deep), constant(deep_x.T), constant(picked), constant(deep_x),
        constant(y_matrix[:, :rows].T), constant(x_matrix),
    )
    if not full:
        total = lax.psum(score, ("gz", "gy"))
        score = cells * total[count:] / (total[:count] * total[:count])
    return denoised, score


def solution(mesh):
    in_specs = (P(("cube", "gz"), "gy", None), P())
    out_specs = (P(("cube", "gz"), None, "gy", None), P("cube"))
    return jax.shard_map(body, mesh=mesh, in_specs=in_specs, out_specs=out_specs, check_vma=False)
```

```python
import functools
import numpy as np
import jax
import jax.numpy as jnp
from jax import lax
from jax.experimental import pallas as pl
from jax.experimental.pallas import tpu as pltpu
from jax.sharding import PartitionSpec as P


LOWPASS = (
    0.2303778133088964,
    0.7148465705529155,
    0.6308807679298587,
    -0.0279837694168599,
    -0.1870348117190931,
    0.0308413818355607,
    0.0328830116668852,
    -0.010597401785069,
)
HIGHPASS = tuple((-1) ** tap * LOWPASS[7 - tap] for tap in range(8))
FILTERS = (LOWPASS, HIGHPASS)


def analysis_matrix(length):
    half = length // 2
    matrix = np.zeros((length, length))
    for band in range(2):
        for k in range(half):
            for tap in range(8):
                matrix[band * half + k, (2 * k + tap) % length] += FILTERS[band][tap]
    return matrix


def dot(a, b):
    return lax.dot_general(
        a, b, (((1,), (0,)), ((), ())),
        precision=lax.Precision.HIGHEST, preferred_element_type=jnp.float32,
    )


def weighted(terms):
    total = None
    for weight, value in terms:
        part = value * weight
        total = part if total is None else total + part
    return total


def depth_kernel(own_ref, before_ref, after_ref, out_ref):
    planes, rows, cols = own_ref.shape
    half_cols = cols // 2
    for r in range(0, rows, 8):
        for c in range(0, cols, half_cols):
            at = (pl.ds(r, 8), pl.ds(c, half_cols))
            tile = [before_ref[(i,) + at] for i in range(planes)]
            tile += [own_ref[(i,) + at] for i in range(planes)]
            tile += [after_ref[(i,) + at] for i in range(2)]
            for k in range(planes // 2):
                for band in range(2):
                    out_ref[(2 * k + band,) + at] = weighted(
                        (FILTERS[band][tap], tile[2 * k + tap]) for tap in range(8)
                    )


def tally(value, limit_squares, sums, keep=None):
    square = value * value
    for t, limit in enumerate(limit_squares):
        weight = 1.0 / (square + limit)
        cut = jnp.minimum(square, limit)
        if keep is not None:
            weight = jnp.where(keep, weight, 0.0)
            cut = jnp.where(keep, cut, 0.0)
        sums[0][t] = weight if sums[0][t] is None else sums[0][t] + weight
        sums[1][t] = cut if sums[1][t] is None else sums[1][t] + cut


def fold(sums):
    rows = [jnp.sum(a, axis=0, keepdims=True) for group in sums for a in group]
    return jnp.concatenate(rows, 0)


def plane_kernel(limits_ref, own_ref, other_ref, y_ref, x_ref, out_ref, tail_ref, parcel_ref, mid):
    planes, rows, cols = own_ref.shape
    out_rows = out_ref.shape[1]
    count = limits_ref.shape[0]
    squares = [limits_ref[t] * limits_ref[t] for t in range(count)]
    half_cols = cols // 2
    lo_rows = rows // 2
    for z in range(planes):
        plane = jnp.concatenate([own_ref[z], other_ref[z]], 0)
        mid[pl.ds(z * out_rows, out_rows), :] = dot(y_ref[...], plane)
    result = dot(mid[...], x_ref[...])
    for z in range(planes):
        out_ref[z] = result[z * out_rows : (z + 1) * out_rows]
    for z in range(2):
        tail_ref[z] = result[(planes - 2 + z) * out_rows : (planes - 1 + z) * out_rows]
    sums = [[None] * count, [None] * count]
    for z in range(planes):
        for r in range(0, 2 * lo_rows, 8):
            for c in range(0, cols, half_cols):
                value = result[z * out_rows + r : z * out_rows + r + 8, c : c + half_cols]
                if z % 2 == 0 and c == 0 and r < lo_rows:
                    parcel_ref[pl.ds(z // 2 * lo_rows + r, 8), :] = value
                else:
                    tally(value, squares, sums)
    parcel_ref[pl.ds(planes // 2 * lo_rows, 2 * count), :] = fold(sums)


def final_kernel(
    full, cells, index_ref, limits_ref, parcels_ref, own_ref, after_ref, tail_ref,
    ya_ref, xa_ref, ysa_ref, xsa_ref, ys_ref, xs_ref,
    out_ref, score_ref, zed, mix, coarse_in, coarse_mid, coarse, wide, wide_y,
):
    planes, rows, cols = own_ref.shape
    count = limits_ref.shape[0]
    half_cols = cols // 2
    limits = [limits_ref[t] for t in range(count)]
    squares = [t * t for t in limits]
    lo_rows = (parcels_ref.shape[2] - 2 * count) // (planes // 2)
    deep_rows = 2 * lo_rows
    pieces = parcels_ref.shape[1]
    depth = planes // 2
    kappas = list(range(-5, -5 + pieces)) if full else list(range(-5, 1))

    def coarse_plane(r, side, i):
        if full:
            r = r % (depth * pieces)
        at = index_ref[r // depth]
        return parcels_ref[side, at, pl.ds((r % depth) * lo_rows + i, 8), :]

    for side in range(2):
        for i in range(0, lo_rows, 8):
            needed = sorted({(2 * kap + 10 + tap) % (depth * pieces) if full else 2 * kap + 10 + tap
                             for kap in kappas for tap in range(8)})
            tile = {r: coarse_plane(r, side, i) for r in needed}
            for a, kap in enumerate(kappas):
                for band in range(2):
                    terms = []
                    for tap in range(8):
                        r = 2 * kap + 10 + tap
                        terms.append((FILTERS[band][tap], tile[r % (depth * pieces) if full else r]))
                    zed[2 * a + band, pl.ds(side * lo_rows + i, 8), :] = weighted(terms)
    for a in range(2 * len(kappas)):
        mix[pl.ds(a * deep_rows, deep_rows), :] = dot(ya_ref[...], zed[a])
    mix[...] = dot(mix[...], xa_ref[...])

    low_lanes = lax.broadcasted_iota(jnp.int32, (8, half_cols), 1) < half_cols // 2
    sums = [[None] * count, [None] * count]
    for a, kap in enumerate(kappas):
        if not full and kap != 0:
            continue
        for band in range(2):
            for i in range(0, deep_rows, 8):
                if not full and i % lo_rows >= lo_rows // 2:
                    continue
                kept = band == 0 and i < lo_rows
                value = mix[pl.ds((2 * a + band) * deep_rows + i, 8), :]
                tally(value, squares, sums, ~low_lanes if kept else None)
    total = fold(sums)
    if full:
        for side in range(2):
            for piece in range(pieces):
                total = total + parcels_ref[side, piece, pl.ds(depth * lo_rows, 2 * count), :]
    else:
        total = total + parcels_ref[0, index_ref[4], pl.ds(depth * lo_rows, 2 * count), :]
    for t in range(count):
        weight = jnp.sum(total[t : t + 1]) * squares[t]
        residual = jnp.sum(total[count + t : count + t + 1])
        if full:
            score_ref[t] = cells * residual / (weight * weight)
        else:
            score_ref[t] = weight
            score_ref[count + t] = residual

    back = [(-2, 1), (-1, 0), (-1, 1), (0, 0), (0, 1)]
    for t in range(count):
        for i in range(0, deep_rows, 8):
            shrunk = {}
            for a, kap in enumerate(kappas):
                if kap > 0:
                    continue
                for band in range(2):
                    value = mix[pl.ds((2 * a + band) * deep_rows + i, 8), :]
                    cut = value - jnp.clip(value, -limits[t], limits[t])
                    if band == 0 and i < lo_rows:
                        cut = jnp.where(low_lanes, value, cut)
                    shrunk[kap, band] = cut
            for b, (p, odd) in enumerate(back):
                coarse_in[t * 5 + b, pl.ds(i, 8), :] = weighted(
                    (FILTERS[band][2 * j + odd], shrunk[p - j, band])
                    for j in range(4) for band in range(2)
                )
    halo_rows = coarse.shape[1]
    for s in range(5 * count):
        coarse_mid[pl.ds(s * halo_rows, halo_rows), :] = dot(ysa_ref[...], coarse_in[s])
    spread = dot(coarse_mid[...], xsa_ref[...])
    for s in range(5 * count):
        coarse[s] = spread[s * halo_rows : (s + 1) * halo_rows]

    def source(kap, band, r, c):
        at = (pl.ds(r, 8), pl.ds(c, half_cols))
        if kap == -3:
            return tail_ref[(band,) + at]
        if kap < 0:
            return own_ref[(2 * (kap + 2) + band,) + at]
        return after_ref[(2 * kap + band,) + at]

    first = lax.broadcasted_iota(jnp.int32, (8, half_cols), 0) < 4
    for r in range(0, rows, 8):
        for c in range(0, cols, half_cols):
            for t in range(count):
                shrunk = {}
                for kap in range(-3, 2):
                    for band in range(2):
                        value = source(kap, band, r, c)
                        cut = value - jnp.clip(value, -limits[t], limits[t])
                        if band == 0 and c == 0:
                            if r < lo_rows:
                                cut = coarse[t * 5 + kap + 3, pl.ds(r, 8), :]
                            elif r >= 2 * lo_rows:
                                low = coarse[t * 5 + kap + 3, pl.ds(lo_rows, 8), :]
                                cut = jnp.where(first, low, cut)
                        shrunk[kap, band] = cut
                for z in range(planes):
                    wide[t * planes + z, pl.ds(r, 8), pl.ds(c, half_cols)] = weighted(
                        (FILTERS[band][2 * j + z % 2], shrunk[z // 2 - j, band])
                        for j in range(4) for band in range(2)
                    )
    y_rows = ys_ref.shape[0]
    for s in range(count * planes):
        wide_y[pl.ds(s * y_rows, y_rows), :] = dot(ys_ref[...], wide[s])
    result = dot(wide_y[...], xs_ref[...])
    for t in range(count):
        for z in range(planes):
            s = t * planes + z
            out_ref[z, t] = result[s * y_rows : (s + 1) * y_rows]


def shifted(array, axis, by):
    devices = lax.axis_size(axis)
    return lax.ppermute(array, axis, [(i, (i + by) % devices) for i in range(devices)])


VMEM = pl.BlockSpec(memory_space=pltpu.VMEM)
SMEM = pl.BlockSpec(memory_space=pltpu.SMEM)
PARAMS = pltpu.CompilerParams(vmem_limit_bytes=24 * 1024 * 1024)


def struct(*shape):
    return jax.ShapeDtypeStruct(shape, jnp.float32)


def constant(matrix):
    return jnp.asarray(np.ascontiguousarray(matrix), jnp.float32)


def body(noisy_cube, thresholds):
    planes, rows, cols = noisy_cube.shape
    count = thresholds.shape[0]
    n = lax.axis_size("gz")
    if lax.axis_size("gy") != 2 or planes != 4:
        raise ValueError("unsupported split")
    lo_rows = rows // 2
    pad = 4
    all_rows = 2 * lo_rows + 2 * pad
    full = n <= 8

    y_all = analysis_matrix(2 * rows)
    y_matrix = np.zeros((all_rows, 2 * rows))
    y_matrix[:lo_rows] = y_all[:lo_rows]
    y_matrix[lo_rows : 2 * lo_rows] = y_all[rows : rows + lo_rows]
    for band in range(2):
        start = 2 * lo_rows + band * pad
        stop = (band + 1) * rows
        y_matrix[start : start + 3] = y_all[stop - 3 : stop]
    x_matrix = analysis_matrix(cols)
    deep = analysis_matrix(rows)
    deep_x = analysis_matrix(cols // 2)
    picked = np.zeros((lo_rows + 8, rows))
    picked[:lo_rows] = deep[:, :lo_rows].T
    picked[lo_rows : lo_rows + 3] = deep[:, rows - 3 :].T

    ahead = shifted(noisy_cube, "gz", 1)
    behind = shifted(noisy_cube[:2], "gz", -1)
    layers = pl.pallas_call(
        depth_kernel,
        out_shape=struct(planes, rows, cols),
        in_specs=[VMEM] * 3,
        out_specs=VMEM,
        compiler_params=PARAMS,
        name="depth",
    )(noisy_cube, ahead, behind)
    other = shifted(layers, "gy", 1)
    own, tail, parcel = pl.pallas_call(
        plane_kernel,
        out_shape=(
            struct(planes, all_rows, cols),
            struct(2, all_rows, cols),
            struct(planes // 2 * lo_rows + 2 * count, cols // 2),
        ),
        in_specs=[SMEM] + [VMEM] * 4,
        out_specs=(VMEM,) * 3,
        scratch_shapes=[pltpu.VMEM((planes * all_rows, cols), jnp.float32)],
        compiler_params=PARAMS,
        name="plane",
    )(thresholds, layers, other, constant(y_matrix), constant(x_matrix.T))

    place = lax.axis_index("gz")
    offsets = jnp.arange(-4, 5)
    if full:
        pairs = n // 2
        column = [parcel]
        for q in range(1, pairs):
            column.append(shifted(parcel, "gz", -2 * q))
        column = jnp.stack(column)
        swapped = lax.ppermute(column, "gz", [(i, i ^ 1) for i in range(n)])
        side = jnp.concatenate([column, swapped])
        inside = place % 2
        spot = (inside + offsets) % n
        index = ((spot % 2) ^ inside) * pairs + spot // 2
    else:
        side = jnp.stack([parcel if o == 0 else shifted(parcel, "gz", -o) for o in range(-4, 5)])
        index = offsets + 4
    parcels = jnp.stack([side, shifted(side, "gy", 1)])
    before = shifted(tail, "gz", 1)
    after = shifted(own, "gz", -1)

    kappas = n if full else 6
    cells = float(planes * rows * cols * n * 2)
    denoised, score = pl.pallas_call(
        functools.partial(final_kernel, full, cells),
        out_shape=(
            struct(planes, count, rows, cols),
            struct(count if full else 2 * count),
        ),
        in_specs=[SMEM] * 2 + [VMEM] * 10,
        out_specs=(VMEM, SMEM),
        scratch_shapes=[
            pltpu.VMEM((2 * kappas, rows, cols // 2), jnp.float32),
            pltpu.VMEM((2 * kappas * rows, cols // 2), jnp.float32),
            pltpu.VMEM((5 * count, rows, cols // 2), jnp.float32),
            pltpu.VMEM((5 * count * (lo_rows + 8), cols // 2), jnp.float32),
            pltpu.VMEM((5 * count, lo_rows + 8, cols // 2), jnp.float32),
            pltpu.VMEM((count * planes, all_rows, cols), jnp.float32),
            pltpu.VMEM((count * planes * rows, cols), jnp.float32),
        ],
        compiler_params=PARAMS,
        name="final",
    )(
        index.astype(jnp.int32), thresholds, parcels, own, after, before,
        constant(deep), constant(deep_x.T), constant(picked), constant(deep_x),
        constant(y_matrix[:, :rows].T), constant(x_matrix),
    )
    if not full:
        total = lax.psum(score, ("gz", "gy"))
        score = cells * total[count:] / (total[:count] * total[:count])
    return denoised, score


def solution(mesh):
    in_specs = (P(("cube", "gz"), "gy", None), P())
    out_specs = (P(("cube", "gz"), None, "gy", None), P("cube"))
    return jax.shard_map(body, mesh=mesh, in_specs=in_specs, out_specs=out_specs, check_vma=False)
```

```python
import functools
import jax
import jax.numpy as jnp
from jax import lax
from jax.experimental import pallas as pl
from jax.experimental.pallas import tpu as pltpu
from jax.sharding import PartitionSpec as P


LOWPASS = (
    0.2303778133088964,
    0.7148465705529155,
    0.6308807679298587,
    -0.0279837694168599,
    -0.1870348117190931,
    0.0308413818355607,
    0.0328830116668852,
    -0.010597401785069,
)
HIGHPASS = tuple((-1) ** tap * LOWPASS[7 - tap] for tap in range(8))
FILTERS = (LOWPASS, HIGHPASS)
EDGE = 8


def dot(a, b, contract=0):
    return lax.dot_general(
        a, b, (((1,), (contract,)), ((), ())),
        precision=lax.Precision.HIGHEST, preferred_element_type=jnp.float32,
    )


def weighted(terms):
    total = None
    for weight, value in terms:
        part = value * weight
        total = part if total is None else total + part
    return total


def filter_tile(first, position, length, band):
    gap = position - first
    gap = jnp.where(gap < 0, gap + length, gap)
    value = jnp.zeros(gap.shape, jnp.float32)
    for tap in range(8):
        value = jnp.where(gap == tap, FILTERS[band][tap], value)
    return value


def iota(shape, dimension):
    return lax.broadcasted_iota(jnp.int32, shape, dimension)


def edge_rows(row, last):
    return last - 2 + row % 4


def analysis_tiles(ref):
    length = ref.shape[0]
    half = length // 2
    for band in range(2):
        shape = (half, length)
        ref[pl.ds(band * half, half), :] = filter_tile(2 * iota(shape, 0), iota(shape, 1), length, band)


def blocks(shape, block):
    row, column = iota(shape, 0), iota(shape, 1)
    return row % block, column % block, row // block == column // block


def first_kernel(cube_ref, x_ref, y_ref, cube_out_ref, semaphore):
    copy = pltpu.make_async_copy(cube_ref, cube_out_ref, semaphore)
    copy.start()
    rows, length = y_ref.shape
    half = rows // 2
    for band in range(2):
        shape = (half, length)
        y_ref[pl.ds(band * half, half), :] = filter_tile(2 * iota(shape, 0), iota(shape, 1), length, band)
    analysis_tiles(x_ref)
    copy.wait()


def second_kernel(x_ref, deep_x_ref, both_x_ref, back_y_ref, deep_y_ref, both_y_ref):
    half_cols = deep_x_ref.shape[0]
    analysis_tiles(deep_x_ref)
    both_x_ref[...] = dot(deep_x_ref[...], x_ref[pl.ds(0, half_cols), :])
    shape = back_y_ref.shape
    rows = shape[0]
    half = rows // 2
    sample, column = iota(shape, 0), iota(shape, 1)
    total = jnp.zeros(shape, jnp.float32)
    for band in range(2):
        value = filter_tile(2 * (column - band * half), sample, 2 * rows, band)
        total = jnp.where((column >= band * half) & (column < (band + 1) * half), value, total)
        start = rows + band * 4
        value = filter_tile(2 * edge_rows(column - start, -1), sample, 2 * rows, band)
        total = jnp.where((column >= start) & (column < start + 3), value, total)
    back_y_ref[...] = total
    row, column, mask = blocks(deep_y_ref.shape, rows)
    first = 2 * jnp.where(row < half, row, row - half)
    lo = filter_tile(first, column, rows, 0)
    hi = filter_tile(first, column, rows, 1)
    deep_y_ref[...] = jnp.where(mask, jnp.where(row < half, lo, hi), 0.0)
    lows = jnp.where(mask, filter_tile(2 * column, row, 2 * rows, 0), 0.0)
    both_y_ref[...] = dot(lows, deep_y_ref[...], 1)


def plane_kernel(flags_ref, own_ref, other_ref, y_ref, x_ref, out_ref, far_ref, mid):
    planes, rows, _ = own_ref.shape
    for z in range(planes):
        plane = jnp.concatenate([own_ref[z], other_ref[z]], 0)
        mid[pl.ds(z * rows, rows), :] = dot(y_ref[...], plane)
    result = dot(mid[...], x_ref[...], 1)
    odd = flags_ref[0] == 1
    for z in range(planes):
        out_ref[z] = result[z * rows : (z + 1) * rows]
    for z in range(2):
        head = result[z * rows : (z + 1) * rows]
        tail = result[(planes - 2 + z) * rows : (planes - 1 + z) * rows]
        far_ref[z] = jnp.where(odd, head, tail)


def tally(value, limit_squares, sums, keep=None):
    square = value * value
    for t, limit in enumerate(limit_squares):
        weight = 1.0 / (square + limit)
        cut = jnp.minimum(square, limit)
        if keep is not None:
            weight = jnp.where(keep, weight, 0.0)
            cut = jnp.where(keep, cut, 0.0)
        sums[0][t] = weight if sums[0][t] is None else sums[0][t] + weight
        sums[1][t] = cut if sums[1][t] is None else sums[1][t] + cut


def fold(sums):
    rows = [jnp.sum(a, axis=0, keepdims=True) for group in sums for a in group]
    return jnp.concatenate(rows, 0)


def depth_kernel(flags_ref, limits_ref, own_ref, mate_ref, level_ref, deep_x_ref, parcel_ref, lows):
    planes, rows, cols = own_ref.shape
    count = limits_ref.shape[0]
    squares = [limits_ref[t] * limits_ref[t] for t in range(count)]
    half_cols = cols // 2
    lo_rows = rows // 2
    odd = flags_ref[0] == 1
    sums = [[None] * count, [None] * count]
    for r in range(0, rows, 8):
        for c in range(0, cols, half_cols):
            at = (pl.ds(r, 8), pl.ds(c, half_cols))
            own = [own_ref[(i,) + at] for i in range(planes)]
            level = [level_ref[(i,) + at] for i in range(planes)]
            tile = [jnp.where(odd, level[i], own[i]) for i in range(planes)]
            tile += [mate_ref[(i,) + at] for i in range(planes)]
            tile += [jnp.where(odd, own[i], level[i]) for i in range(2)]
            for k in range(planes // 2):
                for band in range(2):
                    value = weighted((FILTERS[band][tap], tile[2 * k + tap]) for tap in range(8))
                    if band == 0 and c == 0 and r < lo_rows:
                        lows[pl.ds(k * lo_rows + r, 8), :] = value
                    else:
                        tally(value, squares, sums)
    parcel_ref[pl.ds(0, planes // 2 * lo_rows), :] = dot(lows[...], deep_x_ref[...], 1)
    parcel_ref[pl.ds(planes // 2 * lo_rows, 2 * count), :] = fold(sums)


def stack_kernel(flags_ref, own_ref, mate_ref, level_ref, cross_ref, far_ref, out_ref, edge_ref):
    planes, rows, cols = own_ref.shape
    half_cols = cols // 2
    odd = flags_ref[0] == 1
    for r in range(0, rows, 8):
        for c in range(0, cols, half_cols):
            at = (pl.ds(r, 8), pl.ds(c, half_cols))
            mate = [mate_ref[(i,) + at] for i in range(planes)]
            cross = [cross_ref[(i,) + at] for i in range(planes)]
            level = [level_ref[(i,) + at] for i in range(planes)]
            far = [far_ref[(i,) + at] for i in range(2)]
            tile = [jnp.where(odd, level[planes - 2 + i], far[i]) for i in range(2)]
            tile += [jnp.where(odd, mate[i], cross[i]) for i in range(planes)]
            tile += [own_ref[(i,) + at] for i in range(planes)]
            tile += [jnp.where(odd, cross[i], mate[i]) for i in range(planes)]
            tile += [jnp.where(odd, far[i], level[i]) for i in range(2)]
            for k in range(5):
                for band in range(2):
                    value = weighted((FILTERS[band][tap], tile[2 * k + tap]) for tap in range(8))
                    out_ref[(2 * k + band,) + at] = value
    edge_ref[...] = jnp.zeros(edge_ref.shape, jnp.float32)
    for k in range(10):
        for band in range(2):
            stop = (band + 1) * rows // 2
            edge_ref[k, pl.ds(band * 4, 3), :] = out_ref[k, pl.ds(stop - 3, 3), :]


def detail_kernel(limits_ref, coefs_ref, edge_ref, back_y_ref, x_ref, out_ref, wide, wide_y):
    count, planes = out_ref.shape[0], out_ref.shape[1]
    _, rows, cols = coefs_ref.shape
    half_cols = cols // 2
    lo_rows = rows // 2
    limits = [limits_ref[t] for t in range(count)]
    low_edge = iota((8, half_cols), 0) < 4
    for r in range(0, rows + EDGE, 8):
        for c in range(0, cols, half_cols):
            if r < rows:
                tile = [coefs_ref[i, pl.ds(r, 8), pl.ds(c, half_cols)] for i in range(10)]
            else:
                tile = [edge_ref[i, :, pl.ds(c, half_cols)] for i in range(10)]
            for t in range(count):
                shrunk = {}
                for i, value in enumerate(tile):
                    kap, band = i // 2 - 3, i % 2
                    if band == 0 and c == 0 and r < lo_rows:
                        continue
                    cut = value - jnp.clip(value, -limits[t], limits[t])
                    if band == 0 and c == 0 and r >= rows:
                        cut = jnp.where(low_edge, 0.0, cut)
                    shrunk[kap, band] = cut
                for z in range(planes):
                    wide[t * planes + z, pl.ds(r, 8), pl.ds(c, half_cols)] = weighted(
                        (FILTERS[band][2 * j + z % 2], shrunk[z // 2 - j, band])
                        for j in range(4) for band in range(2) if (z // 2 - j, band) in shrunk
                    )
    for s in range(count * planes):
        wide_y[pl.ds(s * rows, rows), :] = dot(back_y_ref[...], wide[s])
    result = dot(wide_y[...], x_ref[...])
    for t in range(count):
        for z in range(planes):
            s = t * planes + z
            out_ref[t, z] = result[s * rows : (s + 1) * rows]


def way_back(z):
    weights = {}
    for i in range(4):
        plane = z // 2 - i
        for j in range(4):
            for band in range(2):
                at = (plane // 2 - j, band)
                weights[at] = weights.get(at, 0.0) + LOWPASS[2 * i + z % 2] * FILTERS[band][2 * j + plane % 2]
    return weights


def final_kernel(
    full, cells, index_ref, limits_ref, parcels_ref, detail_ref, deep_y_ref, both_y_ref, both_x_ref,
    out_ref, score_ref, zed, mix, coarse,
):
    count, planes, rows, cols = detail_ref.shape
    half_cols = cols // 2
    limits = [limits_ref[t] for t in range(count)]
    squares = [t * t for t in limits]
    depth = planes // 2
    lo_rows = (parcels_ref.shape[2] - 2 * count) // depth
    deep_rows = 2 * lo_rows
    pieces = parcels_ref.shape[1]
    kappas = list(range(-5, -5 + pieces)) if full else list(range(-5, 1))

    def place(kap, tap):
        r = 2 * kap + 10 + tap
        return r % (depth * pieces) if full else r

    for side in range(2):
        for i in range(0, lo_rows, 8):
            tile = {}
            for r in sorted({place(kap, tap) for kap in kappas for tap in range(8)}):
                tile[r] = parcels_ref[side, index_ref[r // depth], pl.ds((r % depth) * lo_rows + i, 8), :]
            for a, kap in enumerate(kappas):
                for band in range(2):
                    zed[pl.ds((2 * a + band) * deep_rows + side * lo_rows + i, 8), :] = weighted(
                        (FILTERS[band][tap], tile[place(kap, tap)]) for tap in range(8)
                    )
    block = deep_y_ref.shape[0]
    for a in range(0, zed.shape[0], block):
        mix[pl.ds(a, block), :] = dot(deep_y_ref[...], zed[pl.ds(a, block), :])

    low_lanes = iota((8, half_cols), 1) < half_cols // 2
    for t in range(count):
        for i in range(0, deep_rows, 8):
            shrunk = {}
            for a, kap in enumerate(kappas):
                if kap > 0:
                    continue
                for band in range(2):
                    value = mix[pl.ds((2 * a + band) * deep_rows + i, 8), :]
                    cut = value - jnp.clip(value, -limits[t], limits[t])
                    if band == 0 and i < lo_rows:
                        cut = jnp.where(low_lanes, value, cut)
                    shrunk[kap, band] = cut
            for z in range(planes):
                coarse[pl.ds((t * planes + z) * rows + i, 8), :] = weighted(
                    (weight, shrunk[at]) for at, weight in way_back(z).items()
                )
        result = dot(both_y_ref[...], coarse[pl.ds(t * block, block), :])
        result = dot(result, both_x_ref[...])
        for z in range(planes):
            out_ref[z, t] = detail_ref[t, z] + result[z * rows : (z + 1) * rows]

    sums = [[None] * count, [None] * count]
    for a, kap in enumerate(kappas):
        if not full and kap != 0:
            continue
        for band in range(2):
            for i in range(0, deep_rows, 8):
                if not full and i % lo_rows >= lo_rows // 2:
                    continue
                kept = band == 0 and i < lo_rows
                value = mix[pl.ds((2 * a + band) * deep_rows + i, 8), :]
                tally(value, squares, sums, ~low_lanes if kept else None)
    total = fold(sums)
    if full:
        for side in range(2):
            for piece in range(pieces):
                total = total + parcels_ref[side, piece, pl.ds(depth * lo_rows, 2 * count), :]
    else:
        total = total + parcels_ref[0, 5, pl.ds(depth * lo_rows, 2 * count), :]
    for t in range(count):
        weight = jnp.sum(total[t : t + 1]) * squares[t]
        residual = jnp.sum(total[count + t : count + t + 1])
        if full:
            score_ref[t] = cells * residual / (weight * weight)
        else:
            score_ref[t] = weight
            score_ref[count + t] = residual


def shifted(array, axis, by):
    devices = lax.axis_size(axis)
    return lax.ppermute(array, axis, [(i, (i + by) % devices) for i in range(devices)])


def exchanged(array, partner):
    devices = lax.axis_size("gz")
    return lax.ppermute(array, "gz", [(i, partner(i) % devices) for i in range(devices)])


VMEM = pl.BlockSpec(memory_space=pltpu.VMEM)
SMEM = pl.BlockSpec(memory_space=pltpu.SMEM)
PARAMS = pltpu.CompilerParams(vmem_limit_bytes=24 * 1024 * 1024)


def struct(*shape):
    return jax.ShapeDtypeStruct(shape, jnp.float32)


def scratch(*shape):
    return pltpu.VMEM(shape, jnp.float32)


def call(kernel, out_shape, smem, vmem, scratches=(), score=False, flops=100_000):
    out_specs = jax.tree.map(lambda _: VMEM, out_shape)
    if score:
        out_specs = (VMEM, SMEM)

    def run(*operands):
        return pl.pallas_call(
            kernel,
            out_shape=out_shape,
            in_specs=[SMEM] * smem + vmem,
            out_specs=out_specs,
            scratch_shapes=list(scratches),
            compiler_params=PARAMS,
            cost_estimate=pl.CostEstimate(flops=flops, bytes_accessed=0, transcendentals=0),
        )(*operands)

    return run


def body(noisy_cube, thresholds):
    planes, rows, cols = noisy_cube.shape
    count = thresholds.shape[0]
    n = lax.axis_size("gz")
    if lax.axis_size("gy") != 2 or planes != 4 or n % 4:
        raise ValueError("unsupported split")
    lo_rows = rows // 2
    half_cols = cols // 2
    full = n <= 8 and n & (n - 1) == 0

    place = lax.axis_index("gz")
    inside = place % 2
    flags = inside.astype(jnp.int32)[None]

    other = shifted(noisy_cube, "gy", 1)
    x_matrix, y_matrix, cube = call(
        first_kernel,
        (
            struct(cols, cols), struct(rows, 2 * rows), struct(planes, rows, cols),
        ), 0, [pl.BlockSpec(memory_space=pltpu.HBM)], [pltpu.SemaphoreType.DMA],
    )(noisy_cube)
    flat, far = call(
        plane_kernel, (struct(planes, rows, cols), struct(2, rows, cols)), 1, [VMEM] * 4,
        [scratch(planes * rows, cols)],
    )(flags, cube, other, y_matrix, x_matrix)

    level = exchanged(flat, lambda i: i + 2 if i % 2 else i - 2)
    mate = exchanged(flat, lambda i: i ^ 1)
    cross = exchanged(flat, lambda i: i + 1 if i % 2 else i - 1)
    far = exchanged(far, lambda i: i - 2 if i % 2 else i + 2)
    deep_x, both_x, back_y, deep_y, both_y = call(
        second_kernel,
        (
            struct(half_cols, half_cols), struct(half_cols, cols), struct(rows, rows + EDGE),
            struct(planes * rows, planes * rows), struct(planes * rows, planes * rows),
        ), 0, [VMEM],
    )(x_matrix)
    parcel = call(
        depth_kernel, struct(planes // 2 * lo_rows + 2 * count, half_cols), 2, [VMEM] * 4,
        [scratch(planes // 2 * lo_rows, half_cols)],
    )(flags, thresholds, flat, mate, level, deep_x)

    spot = place + jnp.arange(-5, 4)
    owner = (spot + 2 * (spot % 2)) % n
    if full:
        pairs = n // 2
        column = [parcel]
        for q in range(1, pairs):
            column.append(exchanged(parcel, lambda i: i ^ 2 * q))
        column = jnp.stack(column)
        swapped = exchanged(column, lambda i: i ^ 1)
        side = jnp.concatenate([column, swapped])
        index = ((owner % 2) ^ inside) * pairs + ((owner // 2) ^ (place // 2))
    else:
        side = jnp.stack([parcel if o == 0 else shifted(parcel, "gz", -o) for o in range(-5, 6)])
        index = spot + 2 * (spot % 2) - place + 5
    parcels = jnp.stack([side, shifted(side, "gy", 1)])

    coefs, edge = call(
        stack_kernel, (struct(10, rows, cols), struct(10, EDGE, cols)), 1, [VMEM] * 5
    )(flags, flat, mate, level, cross, far)
    edge = shifted(edge, "gy", 1)
    detail = call(
        detail_kernel, struct(count, planes, rows, cols), 1, [VMEM] * 4,
        [scratch(count * planes, rows + EDGE, cols), scratch(count * planes * rows, cols)],
        flops=20_000_000,
    )(thresholds, coefs, edge, back_y, x_matrix)

    kappas = n if full else 6
    cells = float(planes * rows * cols * n * 2)
    denoised, score = call(
        functools.partial(final_kernel, full, cells),
        (struct(planes, count, rows, cols), struct(count if full else 2 * count)), 2, [VMEM] * 5,
        [
            scratch(2 * kappas * rows, half_cols),
            scratch(2 * kappas * rows, half_cols),
            scratch(planes * count * rows, half_cols),
        ],
        score=True,
    )(index.astype(jnp.int32), thresholds, parcels, detail, deep_y, both_y, both_x)
    if not full:
        total = lax.psum(score, ("gz", "gy"))
        score = cells * total[count:] / (total[:count] * total[:count])
    return denoised, score


def solution(mesh):
    in_specs = (P(("cube", "gz"), "gy", None), P())
    out_specs = (P(("cube", "gz"), None, "gy", None), P("cube"))
    return jax.shard_map(body, mesh=mesh, in_specs=in_specs, out_specs=out_specs, check_vma=False)
```

```python
import functools
import jax
import jax.numpy as jnp
from jax import lax
from jax.experimental import pallas as pl
from jax.experimental.pallas import tpu as pltpu
from jax.sharding import PartitionSpec as P


LOWPASS = (
    0.2303778133088964,
    0.7148465705529155,
    0.6308807679298587,
    -0.0279837694168599,
    -0.1870348117190931,
    0.0308413818355607,
    0.0328830116668852,
    -0.010597401785069,
)
HIGHPASS = tuple((-1) ** tap * LOWPASS[7 - tap] for tap in range(8))
FILTERS = (LOWPASS, HIGHPASS)
EDGE = 8


def dot(a, b, contract=0):
    return lax.dot_general(
        a, b, (((1,), (contract,)), ((), ())),
        precision=lax.Precision.HIGHEST, preferred_element_type=jnp.float32,
    )


def weighted(terms):
    total = None
    for weight, value in terms:
        part = value * weight
        total = part if total is None else total + part
    return total


def filter_tile(first, position, length, band):
    gap = position - first
    gap = jnp.where(gap < 0, gap + length, gap)
    value = jnp.zeros(gap.shape, jnp.float32)
    for tap in range(8):
        value = jnp.where(gap == tap, FILTERS[band][tap], value)
    return value


def iota(shape, dimension):
    return lax.broadcasted_iota(jnp.int32, shape, dimension)


def edge_rows(row, last):
    return last - 2 + row % 4


def analysis_tiles(ref, across=False):
    length = ref.shape[0]
    half = length // 2
    for band in range(2):
        shape = (length, half) if across else (half, length)
        value = filter_tile(2 * iota(shape, int(across)), iota(shape, 1 - int(across)), length, band)
        if across:
            ref[:, pl.ds(band * half, half)] = value
        else:
            ref[pl.ds(band * half, half), :] = value


def split(value):
    high = value.astype(jnp.bfloat16)
    return high, (value - high.astype(jnp.float32)).astype(jnp.bfloat16)


def split_dot(a, b):
    def part(left, right):
        return lax.dot_general(left, right, (((1,), (0,)), ((), ())), preferred_element_type=jnp.float32)

    return part(a[0], b[0]) + (part(a[0], b[1]) + part(a[1], b[0]))


def blocks(shape, block):
    row, column = iota(shape, 0), iota(shape, 1)
    return row % block, column % block, row // block == column // block


def first_kernel(cube_ref, across_ref, y_ref, cube_out_ref, semaphore):
    copy = pltpu.make_async_copy(cube_ref, cube_out_ref, semaphore)
    copy.start()
    rows, length = y_ref.shape
    half = rows // 2
    for band in range(2):
        shape = (half, length)
        y_ref[pl.ds(band * half, half), :] = filter_tile(2 * iota(shape, 0), iota(shape, 1), length, band)
    analysis_tiles(across_ref, True)
    copy.wait()


def second_kernel(x_ref, deep_across_ref, both_x_ref, back_y_ref, both_y_ref, deep_x, deep_y):
    analysis_tiles(x_ref)
    analysis_tiles(deep_across_ref, True)
    analysis_tiles(deep_x)
    half_cols = deep_x.shape[0]
    both_x_ref[0], both_x_ref[1] = split(dot(deep_x[...], x_ref[pl.ds(0, half_cols), :]))
    shape = back_y_ref.shape
    rows = shape[0]
    half = rows // 2
    sample, column = iota(shape, 0), iota(shape, 1)
    total = jnp.zeros(shape, jnp.float32)
    for band in range(2):
        value = filter_tile(2 * (column - band * half), sample, 2 * rows, band)
        total = jnp.where((column >= band * half) & (column < (band + 1) * half), value, total)
        start = rows + band * 4
        value = filter_tile(2 * edge_rows(column - start, -1), sample, 2 * rows, band)
        total = jnp.where((column >= start) & (column < start + 3), value, total)
    back_y_ref[...] = total
    row, column, mask = blocks(deep_y.shape, rows)
    first = 2 * jnp.where(row < half, row, row - half)
    lo = filter_tile(first, column, rows, 0)
    hi = filter_tile(first, column, rows, 1)
    deep_y[...] = jnp.where(mask, jnp.where(row < half, lo, hi), 0.0)
    lows = jnp.where(mask, filter_tile(2 * column, row, 2 * rows, 0), 0.0)
    both_y_ref[0], both_y_ref[1] = split(dot(lows, deep_y[...], 1))


def plane_kernel(place_ref, own_ref, other_ref, y_ref, x_ref, out_ref, far_ref, mid):
    planes, rows, _ = own_ref.shape
    for z in range(planes):
        plane = jnp.concatenate([own_ref[z], other_ref[z]], 0)
        mid[pl.ds(z * rows, rows), :] = dot(y_ref[...], plane)
    result = dot(mid[...], x_ref[...])
    odd = place_ref[0] % 2 == 1
    for z in range(planes):
        out_ref[z] = result[z * rows : (z + 1) * rows]
    for z in range(2):
        head = result[z * rows : (z + 1) * rows]
        tail = result[(planes - 2 + z) * rows : (planes - 1 + z) * rows]
        far_ref[z] = jnp.where(odd, head, tail)


def tally(value, limit_squares, sums, keep=None):
    square = value * value
    for t, limit in enumerate(limit_squares):
        weight = 1.0 / (square + limit)
        cut = jnp.minimum(square, limit)
        if keep is not None:
            weight = jnp.where(keep, weight, 0.0)
            cut = jnp.where(keep, cut, 0.0)
        sums[0][t] = weight if sums[0][t] is None else sums[0][t] + weight
        sums[1][t] = cut if sums[1][t] is None else sums[1][t] + cut


def fold(sums):
    rows = [jnp.sum(a, axis=0, keepdims=True) for group in sums for a in group]
    return jnp.concatenate(rows, 0)


def depth_kernel(place_ref, limits_ref, own_ref, mate_ref, level_ref, deep_across_ref, parcel_ref, lows):
    planes, rows, cols = own_ref.shape
    count = limits_ref.shape[0]
    squares = [limits_ref[t] * limits_ref[t] for t in range(count)]
    half_cols = cols // 2
    lo_rows = rows // 2
    odd = place_ref[0] % 2 == 1
    sums = [[None] * count, [None] * count]
    for r in range(0, rows, 8):
        for c in range(0, cols, half_cols):
            at = (pl.ds(r, 8), pl.ds(c, half_cols))
            own = [own_ref[(i,) + at] for i in range(planes)]
            level = [level_ref[(i,) + at] for i in range(planes)]
            tile = [jnp.where(odd, level[i], own[i]) for i in range(planes)]
            tile += [mate_ref[(i,) + at] for i in range(planes)]
            tile += [jnp.where(odd, own[i], level[i]) for i in range(2)]
            for k in range(planes // 2):
                for band in range(2):
                    value = weighted((FILTERS[band][tap], tile[2 * k + tap]) for tap in range(8))
                    if band == 0 and c == 0 and r < lo_rows:
                        lows[pl.ds(k * lo_rows + r, 8), :] = value
                    else:
                        tally(value, squares, sums)
    parcel_ref[pl.ds(0, planes // 2 * lo_rows), :] = dot(lows[...], deep_across_ref[...])
    parcel_ref[pl.ds(planes // 2 * lo_rows, 2 * count), :] = fold(sums)


def stack_kernel(place_ref, own_ref, mate_ref, level_ref, cross_ref, far_ref, out_ref, edge_ref):
    planes, rows, cols = own_ref.shape
    half_cols = cols // 2
    odd = place_ref[0] % 2 == 1
    for r in range(0, rows, 8):
        for c in range(0, cols, half_cols):
            at = (pl.ds(r, 8), pl.ds(c, half_cols))
            mate = [mate_ref[(i,) + at] for i in range(planes)]
            cross = [cross_ref[(i,) + at] for i in range(planes)]
            level = [level_ref[(i,) + at] for i in range(planes)]
            far = [far_ref[(i,) + at] for i in range(2)]
            tile = [jnp.where(odd, level[planes - 2 + i], far[i]) for i in range(2)]
            tile += [jnp.where(odd, mate[i], cross[i]) for i in range(planes)]
            tile += [own_ref[(i,) + at] for i in range(planes)]
            tile += [jnp.where(odd, cross[i], mate[i]) for i in range(planes)]
            tile += [jnp.where(odd, far[i], level[i]) for i in range(2)]
            for k in range(5):
                for band in range(2):
                    value = weighted((FILTERS[band][tap], tile[2 * k + tap]) for tap in range(8))
                    out_ref[(2 * k + band,) + at] = value
    edge_ref[...] = jnp.zeros(edge_ref.shape, jnp.float32)
    for k in range(10):
        for band in range(2):
            stop = (band + 1) * rows // 2
            edge_ref[k, pl.ds(band * 4, 3), :] = out_ref[k, pl.ds(stop - 3, 3), :]


def detail_kernel(limits_ref, coefs_ref, edge_ref, back_y_ref, x_ref, out_ref, wide, wide_y):
    count, planes = out_ref.shape[0], out_ref.shape[1]
    _, rows, cols = coefs_ref.shape
    half_cols = cols // 2
    lo_rows = rows // 2
    limits = [limits_ref[t] for t in range(count)]
    low_edge = iota((8, half_cols), 0) < 4
    for r in range(0, rows + EDGE, 8):
        for c in range(0, cols, half_cols):
            if r < rows:
                tile = [coefs_ref[i, pl.ds(r, 8), pl.ds(c, half_cols)] for i in range(10)]
            else:
                tile = [edge_ref[i, :, pl.ds(c, half_cols)] for i in range(10)]
            for t in range(count):
                shrunk = {}
                for i, value in enumerate(tile):
                    kap, band = i // 2 - 3, i % 2
                    if band == 0 and c == 0 and r < lo_rows:
                        continue
                    cut = value - jnp.clip(value, -limits[t], limits[t])
                    if band == 0 and c == 0 and r >= rows:
                        cut = jnp.where(low_edge, 0.0, cut)
                    shrunk[kap, band] = cut
                for z in range(planes):
                    wide[t * planes + z, pl.ds(r, 8), pl.ds(c, half_cols)] = weighted(
                        (FILTERS[band][2 * j + z % 2], shrunk[z // 2 - j, band])
                        for j in range(4) for band in range(2) if (z // 2 - j, band) in shrunk
                    )
    for s in range(count * planes):
        wide_y[pl.ds(s * rows, rows), :] = dot(back_y_ref[...], wide[s])
    result = dot(wide_y[...], x_ref[...])
    for t in range(count):
        for z in range(planes):
            s = t * planes + z
            out_ref[t, z] = result[s * rows : (s + 1) * rows]


def way_back(z):
    weights = {}
    for i in range(4):
        plane = z // 2 - i
        for j in range(4):
            for band in range(2):
                at = (plane // 2 - j, band)
                weights[at] = weights.get(at, 0.0) + LOWPASS[2 * i + z % 2] * FILTERS[band][2 * j + plane % 2]
    return weights


def final_kernel(
    full, cells, place_ref, limits_ref, parcels_ref, detail_ref, both_y_ref, both_x_ref,
    out_ref, score_ref, zed, mix, coarse, staged, semaphores,
):
    count, planes, rows, cols = detail_ref.shape
    half_cols = cols // 2
    limits = [limits_ref[t] for t in range(count)]
    squares = [t * t for t in limits]
    depth = planes // 2
    lo_rows = (parcels_ref.shape[2] - 2 * count) // depth
    deep_rows = 2 * lo_rows
    pieces = parcels_ref.shape[1]
    kappas = list(range(-5, -5 + pieces)) if full else list(range(-5, 1))
    here = place_ref[0]

    def piece(spot):
        spot = here + pieces + spot
        if not full:
            return spot + 2 * (spot % 2) - here - pieces + 5
        owner = (spot + 2 * (spot % 2)) % pieces
        return ((owner % 2) ^ (here % 2)) * (pieces // 2) + ((owner // 2) ^ (here // 2))

    def reach(kap, tap):
        r = 2 * kap + 10 + tap
        return r % (depth * pieces) if full else r

    used = sorted({reach(kap, tap) for kap in kappas for tap in range(8)})
    spots = {r // depth: piece(r // depth - 5) for r in used}
    for side in range(2):
        for i in range(0, lo_rows, 8):
            tile = {r: parcels_ref[side, spots[r // depth], pl.ds((r % depth) * lo_rows + i, 8), :] for r in used}
            for a, kap in enumerate(kappas):
                for band in range(2):
                    value = weighted((FILTERS[band][tap], tile[reach(kap, tap)]) for tap in range(8))
                    zed[2 * a + band, pl.ds(side * lo_rows + i, 8), :] = value
                    if side == 0 and i == 0:
                        zed[2 * a + band, pl.ds(deep_rows, 8), :] = value
    for a in range(2 * len(kappas)):
        for i in range(0, lo_rows, 8):
            tile = [zed[a, pl.ds(2 * i + tap, 8, stride=2), :] for tap in range(8)]
            for band in range(2):
                mix[pl.ds(a * deep_rows + band * lo_rows + i, 8), :] = weighted(zip(FILTERS[band], tile))

    low_lanes = iota((8, half_cols), 1) < half_cols // 2
    block = planes * rows
    both_y = (both_y_ref[0], both_y_ref[1])
    both_x = (both_x_ref[0], both_x_ref[1])
    copies = []
    for t in range(count):
        for i in range(0, deep_rows, 8):
            shrunk = {}
            for a, kap in enumerate(kappas):
                if kap > 0:
                    continue
                for band in range(2):
                    value = mix[pl.ds((2 * a + band) * deep_rows + i, 8), :]
                    cut = value - jnp.clip(value, -limits[t], limits[t])
                    if band == 0 and i < lo_rows:
                        cut = jnp.where(low_lanes, value, cut)
                    shrunk[kap, band] = cut
            for z in range(planes):
                coarse[pl.ds((t * planes + z) * rows + i, 8), :] = weighted(
                    (weight, shrunk[at]) for at, weight in way_back(z).items()
                )
        result = split_dot(both_y, split(coarse[pl.ds(t * block, block), :]))
        result = split_dot(split(result), both_x)
        for z in range(planes):
            staged[t, z] = detail_ref[t, z] + result[z * rows : (z + 1) * rows]
        copies.append(pltpu.make_async_copy(staged.at[t], out_ref.at[:, t], semaphores.at[t]))
        copies[-1].start()

    sums = [[None] * count, [None] * count]
    for a, kap in enumerate(kappas):
        if not full and kap != 0:
            continue
        for band in range(2):
            for i in range(0, deep_rows, 8):
                if not full and i % lo_rows >= lo_rows // 2:
                    continue
                kept = band == 0 and i < lo_rows
                value = mix[pl.ds((2 * a + band) * deep_rows + i, 8), :]
                tally(value, squares, sums, ~low_lanes if kept else None)
    total = fold(sums)
    if full:
        for side in range(2):
            for at in range(pieces):
                total = total + parcels_ref[side, at, pl.ds(depth * lo_rows, 2 * count), :]
    else:
        total = total + parcels_ref[0, 5, pl.ds(depth * lo_rows, 2 * count), :]
    for t in range(count):
        weight = jnp.sum(total[t : t + 1] * squares[t][:1])
        residual = jnp.sum(total[count + t : count + t + 1])
        if full:
            score_ref[t] = cells * residual / (weight * weight)
        else:
            score_ref[t] = weight
            score_ref[count + t] = residual
    for copy in copies:
        copy.wait()


def shifted(array, axis, by):
    devices = lax.axis_size(axis)
    return lax.ppermute(array, axis, [(i, (i + by) % devices) for i in range(devices)])


def exchanged(array, partner):
    devices = lax.axis_size("gz")
    return lax.ppermute(array, "gz", [(i, partner(i) % devices) for i in range(devices)])


VMEM = pl.BlockSpec(memory_space=pltpu.VMEM)
SMEM = pl.BlockSpec(memory_space=pltpu.SMEM)
PARAMS = pltpu.CompilerParams(vmem_limit_bytes=24 * 1024 * 1024)


def struct(*shape):
    return jax.ShapeDtypeStruct(shape, jnp.float32)


def scratch(*shape):
    return pltpu.VMEM(shape, jnp.float32)


def call(kernel, out_shape, smem, vmem, scratches=(), score=False, flops=100_000):
    out_specs = jax.tree.map(lambda _: VMEM, out_shape)
    if score:
        out_specs = (pl.BlockSpec(memory_space=pltpu.HBM), SMEM)

    def run(*operands):
        return pl.pallas_call(
            kernel,
            out_shape=out_shape,
            in_specs=[SMEM] * smem + vmem,
            out_specs=out_specs,
            scratch_shapes=list(scratches),
            compiler_params=PARAMS,
            cost_estimate=pl.CostEstimate(flops=flops, bytes_accessed=0, transcendentals=0),
        )(*operands)

    return run


def body(noisy_cube, thresholds):
    planes, rows, cols = noisy_cube.shape
    count = thresholds.shape[0]
    n = lax.axis_size("gz")
    if lax.axis_size("gy") != 2 or planes != 4 or n % 4:
        raise ValueError("unsupported split")
    lo_rows = rows // 2
    half_cols = cols // 2
    full = n <= 8 and n & (n - 1) == 0

    place = lax.axis_index("gz")
    limits = jnp.broadcast_to(thresholds[:, None, None], (count, 8, half_cols))
    where = place.astype(jnp.int32)[None]

    other = shifted(noisy_cube, "gy", 1)
    across, y_matrix, cube = call(
        first_kernel,
        (
            struct(cols, cols), struct(rows, 2 * rows), struct(planes, rows, cols),
        ), 0, [pl.BlockSpec(memory_space=pltpu.HBM)], [pltpu.SemaphoreType.DMA],
    )(noisy_cube)
    flat, far = call(
        plane_kernel, (struct(planes, rows, cols), struct(2, rows, cols)), 1, [VMEM] * 4,
        [scratch(planes * rows, cols)],
    )(where, cube, other, y_matrix, across)

    level = exchanged(flat, lambda i: i + 2 if i % 2 else i - 2)
    mate = exchanged(flat, lambda i: i ^ 1)
    cross = exchanged(flat, lambda i: i + 1 if i % 2 else i - 1)
    far = exchanged(far, lambda i: i - 2 if i % 2 else i + 2)
    half = functools.partial(jax.ShapeDtypeStruct, dtype=jnp.bfloat16)
    block = planes * rows
    x_matrix, deep_across, both_x, back_y, both_y = call(
        second_kernel,
        (
            struct(cols, cols), struct(half_cols, half_cols), half((2, half_cols, cols)),
            struct(rows, rows + EDGE), half((2, block, block)),
        ), 0, [], [scratch(half_cols, half_cols), scratch(block, block)],
    )()
    parcel = call(
        depth_kernel, struct(planes // 2 * lo_rows + 2 * count, half_cols), 1, [VMEM] * 5,
        [scratch(planes // 2 * lo_rows, half_cols)],
    )(where, limits, flat, mate, level, deep_across)

    if full:
        pairs = n // 2
        column = [parcel]
        for q in range(1, pairs):
            column.append(exchanged(parcel, lambda i: i ^ 2 * q))
        column = jnp.stack(column)
        swapped = exchanged(column, lambda i: i ^ 1)
        side = jnp.concatenate([column, swapped])
    else:
        side = jnp.stack([parcel if o == 0 else shifted(parcel, "gz", -o) for o in range(-5, 6)])
    parcels = jnp.stack([side, shifted(side, "gy", 1)])

    coefs, edge = call(
        stack_kernel, (struct(10, rows, cols), struct(10, EDGE, cols)), 1, [VMEM] * 5
    )(where, flat, mate, level, cross, far)
    edge = shifted(edge, "gy", 1)
    detail = call(
        detail_kernel, struct(count, planes, rows, cols), 0, [VMEM] * 5,
        [scratch(count * planes, rows + EDGE, cols), scratch(count * planes * rows, cols)],
        flops=20_000_000,
    )(limits, coefs, edge, back_y, x_matrix)

    kappas = n if full else 6
    cells = float(planes * rows * cols * n * 2)
    denoised, score = call(
        functools.partial(final_kernel, full, cells),
        (struct(planes, count, rows, cols), struct(count if full else 2 * count)), 1, [VMEM] * 5,
        [
            scratch(2 * kappas, rows + EDGE, half_cols),
            scratch(2 * kappas * rows, half_cols),
            scratch(count * block, half_cols),
            scratch(count, planes, rows, cols),
            pltpu.SemaphoreType.DMA((count,)),
        ],
        score=True,
    )(where, limits, parcels, detail, both_y, both_x)
    if not full:
        total = lax.psum(score, ("gz", "gy"))
        score = cells * total[count:] / (total[:count] * total[:count])
    return denoised, score


def solution(mesh):
    in_specs = (P(("cube", "gz"), "gy", None), P())
    out_specs = (P(("cube", "gz"), None, "gy", None), P("cube"))
    return jax.shard_map(body, mesh=mesh, in_specs=in_specs, out_specs=out_specs, check_vma=False)
```

```python
import functools
import jax
import jax.numpy as jnp
from jax import lax
from jax.experimental import pallas as pl
from jax.experimental.pallas import tpu as pltpu
from jax.sharding import PartitionSpec as P


LOWPASS = (
    0.2303778133088964,
    0.7148465705529155,
    0.6308807679298587,
    -0.0279837694168599,
    -0.1870348117190931,
    0.0308413818355607,
    0.0328830116668852,
    -0.010597401785069,
)
HIGHPASS = tuple((-1) ** tap * LOWPASS[7 - tap] for tap in range(8))
FILTERS = (LOWPASS, HIGHPASS)
EDGE = 8


def dot(a, b, contract=0):
    return lax.dot_general(
        a, b, (((1,), (contract,)), ((), ())),
        precision=lax.Precision.HIGHEST, preferred_element_type=jnp.float32,
    )


def weighted(terms):
    total = None
    for weight, value in terms:
        part = value * weight
        total = part if total is None else total + part
    return total


def filter_tile(first, position, length, band):
    gap = position - first
    gap = jnp.where(gap < 0, gap + length, gap)
    value = jnp.zeros(gap.shape, jnp.float32)
    for tap in range(8):
        value = jnp.where(gap == tap, FILTERS[band][tap], value)
    return value


def iota(shape, dimension):
    return lax.broadcasted_iota(jnp.int32, shape, dimension)


def edge_rows(row, last):
    return last - 2 + row % 4


def analysis_tiles(ref, across=False):
    length = ref.shape[0]
    half = length // 2
    for band in range(2):
        shape = (length, half) if across else (half, length)
        value = filter_tile(2 * iota(shape, int(across)), iota(shape, 1 - int(across)), length, band)
        if across:
            ref[:, pl.ds(band * half, half)] = value
        else:
            ref[pl.ds(band * half, half), :] = value


def split(value):
    high = value.astype(jnp.bfloat16)
    return high, (value - high.astype(jnp.float32)).astype(jnp.bfloat16)


def split_dot(a, b):
    def part(left, right):
        return lax.dot_general(left, right, (((1,), (0,)), ((), ())), preferred_element_type=jnp.float32)

    return part(a[0], b[0]) + (part(a[0], b[1]) + part(a[1], b[0]))


def blocks(shape, block):
    row, column = iota(shape, 0), iota(shape, 1)
    return row % block, column % block, row // block == column // block


def first_kernel(cube_ref, across_ref, y_ref, cube_out_ref, semaphore):
    copy = pltpu.make_async_copy(cube_ref, cube_out_ref, semaphore)
    copy.start()
    rows, length = y_ref.shape
    half = rows // 2
    for band in range(2):
        shape = (half, length)
        y_ref[pl.ds(band * half, half), :] = filter_tile(2 * iota(shape, 0), iota(shape, 1), length, band)
    analysis_tiles(across_ref, True)
    copy.wait()


def second_kernel(x_ref, deep_across_ref, both_x_ref, back_y_ref, both_y_ref, deep_x, deep_y):
    analysis_tiles(x_ref)
    analysis_tiles(deep_across_ref, True)
    analysis_tiles(deep_x)
    half_cols = deep_x.shape[0]
    both_x_ref[0], both_x_ref[1] = split(dot(deep_x[...], x_ref[pl.ds(0, half_cols), :]))
    shape = back_y_ref.shape
    rows = shape[0]
    half = rows // 2
    sample, column = iota(shape, 0), iota(shape, 1)
    total = jnp.zeros(shape, jnp.float32)
    for band in range(2):
        value = filter_tile(2 * (column - band * half), sample, 2 * rows, band)
        total = jnp.where((column >= band * half) & (column < (band + 1) * half), value, total)
        start = rows + band * 4
        value = filter_tile(2 * edge_rows(column - start, -1), sample, 2 * rows, band)
        total = jnp.where((column >= start) & (column < start + 3), value, total)
    back_y_ref[...] = total
    row, column, mask = blocks(deep_y.shape, rows)
    first = 2 * jnp.where(row < half, row, row - half)
    lo = filter_tile(first, column, rows, 0)
    hi = filter_tile(first, column, rows, 1)
    deep_y[...] = jnp.where(mask, jnp.where(row < half, lo, hi), 0.0)
    lows = jnp.where(mask, filter_tile(2 * column, row, 2 * rows, 0), 0.0)
    both_y_ref[0], both_y_ref[1] = split(dot(lows, deep_y[...], 1))


def plane_kernel(place_ref, own_ref, other_ref, y_ref, x_ref, out_ref, far_ref, mid):
    planes, rows, _ = own_ref.shape
    for z in range(planes):
        plane = jnp.concatenate([own_ref[z], other_ref[z]], 0)
        mid[pl.ds(z * rows, rows), :] = dot(y_ref[...], plane)
    result = dot(mid[...], x_ref[...])
    odd = place_ref[0] % 2 == 1
    for z in range(planes):
        out_ref[z] = result[z * rows : (z + 1) * rows]
    for z in range(2):
        head = result[z * rows : (z + 1) * rows]
        tail = result[(planes - 2 + z) * rows : (planes - 1 + z) * rows]
        far_ref[z] = jnp.where(odd, head, tail)


def tally(value, limit_squares, sums, keep=None):
    square = value * value
    for t, limit in enumerate(limit_squares):
        weight = 1.0 / (square + limit)
        cut = jnp.minimum(square, limit)
        if keep is not None:
            weight = jnp.where(keep, weight, 0.0)
            cut = jnp.where(keep, cut, 0.0)
        sums[0][t] = weight if sums[0][t] is None else sums[0][t] + weight
        sums[1][t] = cut if sums[1][t] is None else sums[1][t] + cut


def fold(sums):
    rows = [jnp.sum(a, axis=0, keepdims=True) for group in sums for a in group]
    return jnp.concatenate(rows, 0)


def depth_kernel(place_ref, limits_ref, own_ref, mate_ref, level_ref, deep_across_ref, parcel_ref, lows):
    planes, rows, cols = own_ref.shape
    count = limits_ref.shape[0]
    squares = [limits_ref[t] * limits_ref[t] for t in range(count)]
    half_cols = cols // 2
    lo_rows = rows // 2
    odd = place_ref[0] % 2 == 1
    sums = [[None] * count, [None] * count]
    for r in range(0, rows, 8):
        for c in range(0, cols, half_cols):
            at = (pl.ds(r, 8), pl.ds(c, half_cols))
            own = [own_ref[(i,) + at] for i in range(planes)]
            level = [level_ref[(i,) + at] for i in range(planes)]
            tile = [jnp.where(odd, level[i], own[i]) for i in range(planes)]
            tile += [mate_ref[(i,) + at] for i in range(planes)]
            tile += [jnp.where(odd, own[i], level[i]) for i in range(2)]
            for k in range(planes // 2):
                for band in range(2):
                    value = weighted((FILTERS[band][tap], tile[2 * k + tap]) for tap in range(8))
                    if band == 0 and c == 0 and r < lo_rows:
                        lows[pl.ds(k * lo_rows + r, 8), :] = value
                    else:
                        tally(value, squares, sums)
    parcel_ref[pl.ds(0, planes // 2 * lo_rows), :] = dot(lows[...], deep_across_ref[...])
    parcel_ref[pl.ds(planes // 2 * lo_rows, 2 * count), :] = fold(sums)


def stack_kernel(place_ref, own_ref, mate_ref, level_ref, cross_ref, far_ref, out_ref, edge_ref):
    planes, rows, cols = own_ref.shape
    half_cols = cols // 2
    odd = place_ref[0] % 2 == 1
    for r in range(0, rows, 8):
        for c in range(0, cols, half_cols):
            at = (pl.ds(r, 8), pl.ds(c, half_cols))
            mate = [mate_ref[(i,) + at] for i in range(planes)]
            cross = [cross_ref[(i,) + at] for i in range(planes)]
            level = [level_ref[(i,) + at] for i in range(planes)]
            far = [far_ref[(i,) + at] for i in range(2)]
            tile = [jnp.where(odd, level[planes - 2 + i], far[i]) for i in range(2)]
            tile += [jnp.where(odd, mate[i], cross[i]) for i in range(planes)]
            tile += [own_ref[(i,) + at] for i in range(planes)]
            tile += [jnp.where(odd, cross[i], mate[i]) for i in range(planes)]
            tile += [jnp.where(odd, far[i], level[i]) for i in range(2)]
            for k in range(5):
                for band in range(2):
                    value = weighted((FILTERS[band][tap], tile[2 * k + tap]) for tap in range(8))
                    out_ref[(2 * k + band,) + at] = value
    edge_ref[...] = jnp.zeros(edge_ref.shape, jnp.float32)
    for k in range(10):
        for band in range(2):
            stop = (band + 1) * rows // 2
            edge_ref[k, pl.ds(band * 4, 3), :] = out_ref[k, pl.ds(stop - 3, 3), :]


def detail_kernel(limits_ref, coefs_ref, edge_ref, back_y_ref, x_ref, out_ref, wide, wide_y):
    count, planes = out_ref.shape[0], out_ref.shape[1]
    _, rows, cols = coefs_ref.shape
    half_cols = cols // 2
    lo_rows = rows // 2
    limits = [limits_ref[t] for t in range(count)]
    low_edge = iota((8, half_cols), 0) < 4
    for r in range(0, rows + EDGE, 8):
        for c in range(0, cols, half_cols):
            if r < rows:
                tile = [coefs_ref[i, pl.ds(r, 8), pl.ds(c, half_cols)] for i in range(10)]
            else:
                tile = [edge_ref[i, :, pl.ds(c, half_cols)] for i in range(10)]
            for t in range(count):
                shrunk = {}
                for i, value in enumerate(tile):
                    kap, band = i // 2 - 3, i % 2
                    if band == 0 and c == 0 and r < lo_rows:
                        continue
                    cut = value - jnp.clip(value, -limits[t], limits[t])
                    if band == 0 and c == 0 and r >= rows:
                        cut = jnp.where(low_edge, 0.0, cut)
                    shrunk[kap, band] = cut
                for z in range(planes):
                    wide[t * planes + z, pl.ds(r, 8), pl.ds(c, half_cols)] = weighted(
                        (FILTERS[band][2 * j + z % 2], shrunk[z // 2 - j, band])
                        for j in range(4) for band in range(2) if (z // 2 - j, band) in shrunk
                    )
    for s in range(count * planes):
        wide_y[pl.ds(s * rows, rows), :] = dot(back_y_ref[...], wide[s])
    result = dot(wide_y[...], x_ref[...])
    for t in range(count):
        for z in range(planes):
            s = t * planes + z
            out_ref[t, z] = result[s * rows : (s + 1) * rows]


def way_back(z):
    weights = {}
    for i in range(4):
        plane = z // 2 - i
        for j in range(4):
            for band in range(2):
                at = (plane // 2 - j, band)
                weights[at] = weights.get(at, 0.0) + LOWPASS[2 * i + z % 2] * FILTERS[band][2 * j + plane % 2]
    return weights


def final_kernel(
    full, cells, place_ref, limits_ref, parcels_ref, detail_ref, both_y_ref, both_x_ref,
    out_ref, score_ref, zed, mix, coarse, staged, semaphores,
):
    count, planes, rows, cols = detail_ref.shape
    half_cols = cols // 2
    limits = [limits_ref[t] for t in range(count)]
    squares = [t * t for t in limits]
    depth = planes // 2
    lo_rows = (parcels_ref.shape[2] - 2 * count) // depth
    deep_rows = 2 * lo_rows
    pieces = parcels_ref.shape[1]
    kappas = list(range(-5, -5 + pieces)) if full else list(range(-5, 1))
    here = place_ref[0]

    def piece(spot):
        spot = here + pieces + spot
        if not full:
            return spot + 2 * (spot % 2) - here - pieces + 5
        owner = (spot + 2 * (spot % 2)) % pieces
        return ((owner // 2) ^ (here // 2)) * 2 + ((owner % 2) ^ (here % 2))

    def reach(kap, tap):
        r = 2 * kap + 10 + tap
        return r % (depth * pieces) if full else r

    used = sorted({reach(kap, tap) for kap in kappas for tap in range(8)})
    spots = {r // depth: piece(r // depth - 5) for r in used}
    for side in range(2):
        for i in range(0, lo_rows, 8):
            tile = {r: parcels_ref[side, spots[r // depth], pl.ds((r % depth) * lo_rows + i, 8), :] for r in used}
            for a, kap in enumerate(kappas):
                for band in range(2):
                    value = weighted((FILTERS[band][tap], tile[reach(kap, tap)]) for tap in range(8))
                    zed[2 * a + band, pl.ds(side * lo_rows + i, 8), :] = value
                    if side == 0 and i == 0:
                        zed[2 * a + band, pl.ds(deep_rows, 8), :] = value
    for a in range(2 * len(kappas)):
        for i in range(0, lo_rows, 8):
            tile = [zed[a, pl.ds(2 * i + tap, 8, stride=2), :] for tap in range(8)]
            for band in range(2):
                mix[pl.ds(a * deep_rows + band * lo_rows + i, 8), :] = weighted(zip(FILTERS[band], tile))

    low_lanes = iota((8, half_cols), 1) < half_cols // 2
    block = planes * rows
    both_y = (both_y_ref[0], both_y_ref[1])
    both_x = (both_x_ref[0], both_x_ref[1])
    copies = []
    for t in range(count):
        for i in range(0, deep_rows, 8):
            shrunk = {}
            for a, kap in enumerate(kappas):
                if kap > 0:
                    continue
                for band in range(2):
                    value = mix[pl.ds((2 * a + band) * deep_rows + i, 8), :]
                    cut = value - jnp.clip(value, -limits[t], limits[t])
                    if band == 0 and i < lo_rows:
                        cut = jnp.where(low_lanes, value, cut)
                    shrunk[kap, band] = cut
            for z in range(planes):
                coarse[pl.ds((t * planes + z) * rows + i, 8), :] = weighted(
                    (weight, shrunk[at]) for at, weight in way_back(z).items()
                )
        result = split_dot(both_y, split(coarse[pl.ds(t * block, block), :]))
        result = split_dot(split(result), both_x)
        for z in range(planes):
            staged[t, z] = detail_ref[t, z] + result[z * rows : (z + 1) * rows]
        copies.append(pltpu.make_async_copy(staged.at[t], out_ref.at[:, t], semaphores.at[t]))
        copies[-1].start()

    sums = [[None] * count, [None] * count]
    for a, kap in enumerate(kappas):
        if not full and kap != 0:
            continue
        for band in range(2):
            for i in range(0, deep_rows, 8):
                if not full and i % lo_rows >= lo_rows // 2:
                    continue
                kept = band == 0 and i < lo_rows
                value = mix[pl.ds((2 * a + band) * deep_rows + i, 8), :]
                tally(value, squares, sums, ~low_lanes if kept else None)
    total = fold(sums)
    if full:
        for side in range(2):
            for at in range(pieces):
                total = total + parcels_ref[side, at, pl.ds(depth * lo_rows, 2 * count), :]
    else:
        total = total + parcels_ref[0, 5, pl.ds(depth * lo_rows, 2 * count), :]
    for t in range(count):
        weight = jnp.sum(total[t : t + 1] * squares[t][:1])
        residual = jnp.sum(total[count + t : count + t + 1])
        if full:
            score_ref[t] = cells * residual / (weight * weight)
        else:
            score_ref[t] = weight
            score_ref[count + t] = residual
    for copy in copies:
        copy.wait()


def shifted(array, axis, by):
    devices = lax.axis_size(axis)
    return lax.ppermute(array, axis, [(i, (i + by) % devices) for i in range(devices)])


def exchanged(array, partner):
    devices = lax.axis_size("gz")
    return lax.ppermute(array, "gz", [(i, partner(i) % devices) for i in range(devices)])


VMEM = pl.BlockSpec(memory_space=pltpu.VMEM)
SMEM = pl.BlockSpec(memory_space=pltpu.SMEM)
PARAMS = pltpu.CompilerParams(vmem_limit_bytes=24 * 1024 * 1024)


def struct(*shape):
    return jax.ShapeDtypeStruct(shape, jnp.float32)


def scratch(*shape):
    return pltpu.VMEM(shape, jnp.float32)


def call(kernel, out_shape, smem, vmem, scratches=(), score=False, flops=100_000):
    out_specs = jax.tree.map(lambda _: VMEM, out_shape)
    if score:
        out_specs = (pl.BlockSpec(memory_space=pltpu.HBM), SMEM)

    def run(*operands):
        return pl.pallas_call(
            kernel,
            out_shape=out_shape,
            in_specs=[SMEM] * smem + vmem,
            out_specs=out_specs,
            scratch_shapes=list(scratches),
            compiler_params=PARAMS,
            cost_estimate=pl.CostEstimate(flops=flops, bytes_accessed=0, transcendentals=0),
        )(*operands)

    return run


def body(noisy_cube, thresholds):
    planes, rows, cols = noisy_cube.shape
    count = thresholds.shape[0]
    n = lax.axis_size("gz")
    if lax.axis_size("gy") != 2 or planes != 4 or n % 4:
        raise ValueError("unsupported split")
    lo_rows = rows // 2
    half_cols = cols // 2
    full = n <= 8 and n & (n - 1) == 0

    place = lax.axis_index("gz")
    limits = jnp.broadcast_to(thresholds[:, None, None], (count, 8, half_cols))
    where = place.astype(jnp.int32)[None]

    other = shifted(noisy_cube, "gy", 1)
    across, y_matrix, cube = call(
        first_kernel,
        (
            struct(cols, cols), struct(rows, 2 * rows), struct(planes, rows, cols),
        ), 0, [pl.BlockSpec(memory_space=pltpu.HBM)], [pltpu.SemaphoreType.DMA],
    )(noisy_cube)
    flat, far = call(
        plane_kernel, (struct(planes, rows, cols), struct(2, rows, cols)), 1, [VMEM] * 4,
        [scratch(planes * rows, cols)],
    )(where, cube, other, y_matrix, across)

    level = exchanged(flat, lambda i: i + 2 if i % 2 else i - 2)
    mate = exchanged(flat, lambda i: i ^ 1)
    far = exchanged(far, lambda i: i - 2 if i % 2 else i + 2)
    half = functools.partial(jax.ShapeDtypeStruct, dtype=jnp.bfloat16)
    block = planes * rows
    x_matrix, deep_across, both_x, back_y, both_y = call(
        second_kernel,
        (
            struct(cols, cols), struct(half_cols, half_cols), half((2, half_cols, cols)),
            struct(rows, rows + EDGE), half((2, block, block)),
        ), 0, [], [scratch(half_cols, half_cols), scratch(block, block)],
    )()
    parcel = call(
        depth_kernel, struct(planes // 2 * lo_rows + 2 * count, half_cols), 1, [VMEM] * 5,
        [scratch(planes // 2 * lo_rows, half_cols)],
    )(where, limits, flat, mate, level, deep_across)

    if full:
        pairs = n // 2
        column = jnp.stack([parcel, exchanged(parcel, lambda i: i ^ 1)])
        side = [column]
        for q in range(1, pairs):
            side.append(exchanged(column, lambda i: i ^ 2 * q))
        side = jnp.concatenate(side)
    else:
        side = jnp.stack([parcel if o == 0 else shifted(parcel, "gz", -o) for o in range(-5, 6)])
    parcels = jnp.stack([side, shifted(side, "gy", 1)])

    cross = exchanged(level, lambda i: i ^ 1)
    coefs, edge = call(
        stack_kernel, (struct(10, rows, cols), struct(10, EDGE, cols)), 1, [VMEM] * 5
    )(where, flat, mate, level, cross, far)
    edge = shifted(edge, "gy", 1)
    detail = call(
        detail_kernel, struct(count, planes, rows, cols), 0, [VMEM] * 5,
        [scratch(count * planes, rows + EDGE, cols), scratch(count * planes * rows, cols)],
        flops=20_000_000,
    )(limits, coefs, edge, back_y, x_matrix)

    kappas = n if full else 6
    cells = float(planes * rows * cols * n * 2)
    denoised, score = call(
        functools.partial(final_kernel, full, cells),
        (struct(planes, count, rows, cols), struct(count if full else 2 * count)), 1, [VMEM] * 5,
        [
            scratch(2 * kappas, rows + EDGE, half_cols),
            scratch(2 * kappas * rows, half_cols),
            scratch(count * block, half_cols),
            scratch(count, planes, rows, cols),
            pltpu.SemaphoreType.DMA((count,)),
        ],
        score=True,
    )(where, limits, parcels, detail, both_y, both_x)
    if not full:
        total = lax.psum(score, ("gz", "gy"))
        score = cells * total[count:] / (total[:count] * total[:count])
    return denoised, score


def solution(mesh):
    in_specs = (P(("cube", "gz"), "gy", None), P())
    out_specs = (P(("cube", "gz"), None, "gy", None), P("cube"))
    return jax.shard_map(body, mesh=mesh, in_specs=in_specs, out_specs=out_specs, check_vma=False)
```

```python
import functools
import jax
import jax.numpy as jnp
from jax import lax
from jax.experimental import pallas as pl
from jax.experimental.pallas import tpu as pltpu
from jax.sharding import PartitionSpec as P


LOWPASS = (
    0.2303778133088964,
    0.7148465705529155,
    0.6308807679298587,
    -0.0279837694168599,
    -0.1870348117190931,
    0.0308413818355607,
    0.0328830116668852,
    -0.010597401785069,
)
HIGHPASS = tuple((-1) ** tap * LOWPASS[7 - tap] for tap in range(8))
FILTERS = (LOWPASS, HIGHPASS)
EDGE = 8


def dot(a, b, contract=0):
    return lax.dot_general(
        a, b, (((1,), (contract,)), ((), ())),
        precision=lax.Precision.HIGHEST, preferred_element_type=jnp.float32,
    )


def weighted(terms):
    total = None
    for weight, value in terms:
        part = value * weight
        total = part if total is None else total + part
    return total


def filter_tile(first, position, length, band):
    gap = position - first
    gap = jnp.where(gap < 0, gap + length, gap)
    value = jnp.zeros(gap.shape, jnp.float32)
    for tap in range(8):
        value = jnp.where(gap == tap, FILTERS[band][tap], value)
    return value


def iota(shape, dimension):
    return lax.broadcasted_iota(jnp.int32, shape, dimension)


def edge_rows(row, last):
    return last - 2 + row % 4


def analysis_tiles(ref, across=False):
    length = ref.shape[0]
    half = length // 2
    for band in range(2):
        shape = (length, half) if across else (half, length)
        value = filter_tile(2 * iota(shape, int(across)), iota(shape, 1 - int(across)), length, band)
        if across:
            ref[:, pl.ds(band * half, half)] = value
        else:
            ref[pl.ds(band * half, half), :] = value


def split(value):
    high = value.astype(jnp.bfloat16)
    return high, (value - high.astype(jnp.float32)).astype(jnp.bfloat16)


def split_dot(a, b):
    def part(left, right):
        return lax.dot_general(left, right, (((1,), (0,)), ((), ())), preferred_element_type=jnp.float32)

    return part(a[0], b[0]) + (part(a[0], b[1]) + part(a[1], b[0]))


def blocks(shape, block):
    row, column = iota(shape, 0), iota(shape, 1)
    return row % block, column % block, row // block == column // block


def first_kernel(cube_ref, across_ref, y_ref, cube_out_ref, semaphore):
    copy = pltpu.make_async_copy(cube_ref, cube_out_ref, semaphore)
    copy.start()
    rows, length = y_ref.shape
    half = rows // 2
    for band in range(2):
        shape = (half, length)
        y_ref[pl.ds(band * half, half), :] = filter_tile(2 * iota(shape, 0), iota(shape, 1), length, band)
    analysis_tiles(across_ref, True)
    copy.wait()


def second_kernel(x_ref, deep_across_ref, both_x_ref, back_y_ref, both_y_ref, deep_x, deep_y):
    analysis_tiles(x_ref)
    analysis_tiles(deep_across_ref, True)
    analysis_tiles(deep_x)
    half_cols = deep_x.shape[0]
    both_x_ref[0], both_x_ref[1] = split(dot(deep_x[...], x_ref[pl.ds(0, half_cols), :]))
    shape = back_y_ref.shape
    rows = shape[0]
    half = rows // 2
    sample, column = iota(shape, 0), iota(shape, 1)
    total = jnp.zeros(shape, jnp.float32)
    for band in range(2):
        value = filter_tile(2 * (column - band * half), sample, 2 * rows, band)
        total = jnp.where((column >= band * half) & (column < (band + 1) * half), value, total)
        start = rows + band * 4
        value = filter_tile(2 * edge_rows(column - start, -1), sample, 2 * rows, band)
        total = jnp.where((column >= start) & (column < start + 3), value, total)
    back_y_ref[...] = total
    row, column, mask = blocks(deep_y.shape, rows)
    first = 2 * jnp.where(row < half, row, row - half)
    lo = filter_tile(first, column, rows, 0)
    hi = filter_tile(first, column, rows, 1)
    deep_y[...] = jnp.where(mask, jnp.where(row < half, lo, hi), 0.0)
    lows = jnp.where(mask, filter_tile(2 * column, row, 2 * rows, 0), 0.0)
    both_y_ref[0], both_y_ref[1] = split(dot(lows, deep_y[...], 1))


def plane_kernel(place_ref, own_ref, other_ref, y_ref, x_ref, out_ref, far_ref, mid):
    planes, rows, _ = own_ref.shape
    for z in range(planes):
        plane = jnp.concatenate([own_ref[z], other_ref[z]], 0)
        mid[pl.ds(z * rows, rows), :] = dot(y_ref[...], plane)
    result = dot(mid[...], x_ref[...])
    odd = place_ref[0] % 2 == 1
    for z in range(planes):
        out_ref[z] = result[z * rows : (z + 1) * rows]
    for z in range(2):
        head = result[z * rows : (z + 1) * rows]
        tail = result[(planes - 2 + z) * rows : (planes - 1 + z) * rows]
        far_ref[z] = jnp.where(odd, head, tail)


def tally(values, limit_squares, sums, keep=None):
    parts = [value * value for value in values]
    for t, limit in enumerate(limit_squares):
        bases = [part + limit for part in parts]
        cuts = [jnp.minimum(part, limit) for part in parts]
        tops = [1.0] * len(bases)
        while len(bases) > 1:
            tops = [tops[i] * bases[i + 1] + tops[i + 1] * bases[i] for i in range(0, len(bases), 2)]
            bases = [bases[i] * bases[i + 1] for i in range(0, len(bases), 2)]
        weight = tops[0] / bases[0]
        cut = functools.reduce(jnp.add, cuts)
        if keep is not None:
            weight = jnp.where(keep, weight, 0.0)
            cut = jnp.where(keep, cut, 0.0)
        sums[0][t] = weight if sums[0][t] is None else sums[0][t] + weight
        sums[1][t] = cut if sums[1][t] is None else sums[1][t] + cut


def fold(sums):
    rows = [jnp.sum(a, axis=0, keepdims=True) for group in sums for a in group]
    return jnp.concatenate(rows, 0)


def depth_kernel(place_ref, limits_ref, own_ref, mate_ref, level_ref, deep_across_ref, parcel_ref, lows):
    planes, rows, cols = own_ref.shape
    count = limits_ref.shape[0]
    squares = [limits_ref[t] * limits_ref[t] for t in range(count)]
    half_cols = cols // 2
    lo_rows = rows // 2
    odd = place_ref[0] % 2 == 1
    sums = [[None] * count, [None] * count]
    for r in range(0, rows, 8):
        for c in range(0, cols, half_cols):
            at = (pl.ds(r, 8), pl.ds(c, half_cols))
            own = [own_ref[(i,) + at] for i in range(planes)]
            level = [level_ref[(i,) + at] for i in range(planes)]
            tile = [jnp.where(odd, level[i], own[i]) for i in range(planes)]
            tile += [mate_ref[(i,) + at] for i in range(planes)]
            tile += [jnp.where(odd, own[i], level[i]) for i in range(2)]
            counted = []
            for k in range(planes // 2):
                for band in range(2):
                    value = weighted((FILTERS[band][tap], tile[2 * k + tap]) for tap in range(8))
                    if band == 0 and c == 0 and r < lo_rows:
                        lows[pl.ds(k * lo_rows + r, 8), :] = value
                    else:
                        counted.append(value)
            tally(counted, squares, sums)
    parcel_ref[pl.ds(0, planes // 2 * lo_rows), :] = dot(lows[...], deep_across_ref[...])
    parcel_ref[pl.ds(planes // 2 * lo_rows, 2 * count), :] = fold(sums)


def stack_kernel(place_ref, own_ref, mate_ref, level_ref, cross_ref, far_ref, out_ref, edge_ref):
    planes, rows, cols = own_ref.shape
    half_cols = cols // 2
    odd = place_ref[0] % 2 == 1
    for r in range(0, rows, 8):
        for c in range(0, cols, half_cols):
            at = (pl.ds(r, 8), pl.ds(c, half_cols))
            mate = [mate_ref[(i,) + at] for i in range(planes)]
            cross = [cross_ref[(i,) + at] for i in range(planes)]
            level = [level_ref[(i,) + at] for i in range(planes)]
            far = [far_ref[(i,) + at] for i in range(2)]
            tile = [jnp.where(odd, level[planes - 2 + i], far[i]) for i in range(2)]
            tile += [jnp.where(odd, mate[i], cross[i]) for i in range(planes)]
            tile += [own_ref[(i,) + at] for i in range(planes)]
            tile += [jnp.where(odd, cross[i], mate[i]) for i in range(planes)]
            tile += [jnp.where(odd, far[i], level[i]) for i in range(2)]
            for k in range(5):
                for band in range(2):
                    value = weighted((FILTERS[band][tap], tile[2 * k + tap]) for tap in range(8))
                    out_ref[(2 * k + band,) + at] = value
    edge_ref[...] = jnp.zeros(edge_ref.shape, jnp.float32)
    for k in range(10):
        for band in range(2):
            stop = (band + 1) * rows // 2
            edge_ref[k, pl.ds(band * 4, 3), :] = out_ref[k, pl.ds(stop - 3, 3), :]


def detail_kernel(limits_ref, coefs_ref, edge_ref, back_y_ref, x_ref, out_ref, wide, wide_y):
    count, planes = out_ref.shape[0], out_ref.shape[1]
    _, rows, cols = coefs_ref.shape
    half_cols = cols // 2
    lo_rows = rows // 2
    limits = [limits_ref[t] for t in range(count)]
    low_edge = iota((8, half_cols), 0) < 4
    for r in range(0, rows + EDGE, 8):
        for c in range(0, cols, half_cols):
            if r < rows:
                tile = [coefs_ref[i, pl.ds(r, 8), pl.ds(c, half_cols)] for i in range(10)]
            else:
                tile = [edge_ref[i, :, pl.ds(c, half_cols)] for i in range(10)]
            for t in range(count):
                shrunk = {}
                for i, value in enumerate(tile):
                    kap, band = i // 2 - 3, i % 2
                    if band == 0 and c == 0 and r < lo_rows:
                        continue
                    cut = value - jnp.clip(value, -limits[t], limits[t])
                    if band == 0 and c == 0 and r >= rows:
                        cut = jnp.where(low_edge, 0.0, cut)
                    shrunk[kap, band] = cut
                for z in range(planes):
                    wide[t * planes + z, pl.ds(r, 8), pl.ds(c, half_cols)] = weighted(
                        (FILTERS[band][2 * j + z % 2], shrunk[z // 2 - j, band])
                        for j in range(4) for band in range(2) if (z // 2 - j, band) in shrunk
                    )
    for s in range(count * planes):
        wide_y[pl.ds(s * rows, rows), :] = dot(back_y_ref[...], wide[s])
    result = dot(wide_y[...], x_ref[...])
    for t in range(count):
        for z in range(planes):
            s = t * planes + z
            out_ref[t, z] = result[s * rows : (s + 1) * rows]


def way_back(z):
    weights = {}
    for i in range(4):
        plane = z // 2 - i
        for j in range(4):
            for band in range(2):
                at = (plane // 2 - j, band)
                weights[at] = weights.get(at, 0.0) + LOWPASS[2 * i + z % 2] * FILTERS[band][2 * j + plane % 2]
    return weights


def final_kernel(
    full, cells, place_ref, limits_ref, parcels_ref, detail_ref, both_y_ref, both_x_ref,
    out_ref, score_ref, zed, mix, coarse, staged, scores, semaphores,
):
    count, planes, rows, cols = detail_ref.shape
    half_cols = cols // 2
    limits = [limits_ref[t] for t in range(count)]
    squares = [t * t for t in limits]
    depth = planes // 2
    lo_rows = (parcels_ref.shape[2] - 2 * count) // depth
    deep_rows = 2 * lo_rows
    pieces = parcels_ref.shape[1]
    kappas = list(range(-5, -5 + pieces)) if full else list(range(-5, 1))
    here = place_ref[0]

    def piece(spot):
        spot = here + pieces + spot
        if not full:
            return spot + 2 * (spot % 2) - here - pieces + 5
        owner = (spot + 2 * (spot % 2)) % pieces
        return ((owner // 2) ^ (here // 2)) * 2 + ((owner % 2) ^ (here % 2))

    def reach(kap, tap):
        r = 2 * kap + 10 + tap
        return r % (depth * pieces) if full else r

    used = sorted({reach(kap, tap) for kap in kappas for tap in range(8)})
    spots = {r // depth: piece(r // depth - 5) for r in used}
    for side in range(2):
        for i in range(0, lo_rows, 8):
            tile = {r: parcels_ref[side, spots[r // depth], pl.ds((r % depth) * lo_rows + i, 8), :] for r in used}
            for a, kap in enumerate(kappas):
                for band in range(2):
                    value = weighted((FILTERS[band][tap], tile[reach(kap, tap)]) for tap in range(8))
                    zed[2 * a + band, pl.ds(side * lo_rows + i, 8), :] = value
                    if side == 0 and i == 0:
                        zed[2 * a + band, pl.ds(deep_rows, 8), :] = value
    for a in range(2 * len(kappas)):
        for i in range(0, lo_rows, 8):
            tile = [zed[a, pl.ds(2 * i + tap, 8, stride=2), :] for tap in range(8)]
            for band in range(2):
                mix[pl.ds(a * deep_rows + band * lo_rows + i, 8), :] = weighted(zip(FILTERS[band], tile))

    low_lanes = iota((8, half_cols), 1) < half_cols // 2
    block = planes * rows
    both_y = (both_y_ref[0], both_y_ref[1])
    both_x = (both_x_ref[0], both_x_ref[1])
    copies = []
    for t in range(count):
        for i in range(0, deep_rows, 8):
            shrunk = {}
            for a, kap in enumerate(kappas):
                if kap > 0:
                    continue
                for band in range(2):
                    value = mix[pl.ds((2 * a + band) * deep_rows + i, 8), :]
                    cut = value - jnp.clip(value, -limits[t], limits[t])
                    if band == 0 and i < lo_rows:
                        cut = jnp.where(low_lanes, value, cut)
                    shrunk[kap, band] = cut
            for z in range(planes):
                coarse[pl.ds((t * planes + z) * rows + i, 8), :] = weighted(
                    (weight, shrunk[at]) for at, weight in way_back(z).items()
                )
        result = split_dot(both_y, split(coarse[pl.ds(t * block, block), :]))
        result = split_dot(split(result), both_x)
        for z in range(planes):
            staged[t, z] = detail_ref[t, z] + result[z * rows : (z + 1) * rows]
        copies.append(pltpu.make_async_copy(staged.at[t], out_ref.at[:, t], semaphores.at[t]))
        copies[-1].start()

    sums = [[None] * count, [None] * count]
    for a, kap in enumerate(kappas):
        if not full and kap != 0:
            continue
        counted = []
        for band in range(2):
            for i in range(0, deep_rows, 8):
                if not full and i % lo_rows >= lo_rows // 2:
                    continue
                value = mix[pl.ds((2 * a + band) * deep_rows + i, 8), :]
                if band == 0 and i < lo_rows:
                    tally([value], squares, sums, ~low_lanes)
                else:
                    counted.append(value)
        for i in range(0, len(counted), 2):
            tally(counted[i : i + 2], squares, sums)
    total = fold(sums)
    if full:
        for side in range(2):
            for at in range(pieces):
                total = total + parcels_ref[side, at, pl.ds(depth * lo_rows, 2 * count), :]
    else:
        total = total + parcels_ref[0, 5, pl.ds(depth * lo_rows, 2 * count), :]
    for t in range(count):
        weight = jnp.sum(total[t : t + 1] * squares[t][:1])
        residual = jnp.sum(total[count + t : count + t + 1])
        if full:
            scores[t] = cells * residual / (weight * weight)
        else:
            scores[t] = weight
            scores[count + t] = residual
    copies.append(pltpu.make_async_copy(scores, score_ref, semaphores.at[count]))
    copies[-1].start()
    for copy in copies:
        copy.wait()


def shifted(array, axis, by):
    devices = lax.axis_size(axis)
    return lax.ppermute(array, axis, [(i, (i + by) % devices) for i in range(devices)])


def exchanged(array, partner):
    devices = lax.axis_size("gz")
    return lax.ppermute(array, "gz", [(i, partner(i) % devices) for i in range(devices)])


VMEM = pl.BlockSpec(memory_space=pltpu.VMEM)
SMEM = pl.BlockSpec(memory_space=pltpu.SMEM)
PARAMS = pltpu.CompilerParams(vmem_limit_bytes=24 * 1024 * 1024)


def struct(*shape):
    return jax.ShapeDtypeStruct(shape, jnp.float32)


def scratch(*shape):
    return pltpu.VMEM(shape, jnp.float32)


def call(kernel, out_shape, smem, vmem, scratches=(), score=False, flops=100_000):
    out_specs = jax.tree.map(lambda _: VMEM, out_shape)
    if score:
        out_specs = (pl.BlockSpec(memory_space=pltpu.HBM),) * 2

    def run(*operands):
        return pl.pallas_call(
            kernel,
            out_shape=out_shape,
            in_specs=[SMEM] * smem + vmem,
            out_specs=out_specs,
            scratch_shapes=list(scratches),
            compiler_params=PARAMS,
            cost_estimate=pl.CostEstimate(flops=flops, bytes_accessed=0, transcendentals=0),
        )(*operands)

    return run


def body(noisy_cube, thresholds):
    planes, rows, cols = noisy_cube.shape
    count = thresholds.shape[0]
    n = lax.axis_size("gz")
    if lax.axis_size("gy") != 2 or planes != 4 or n % 4:
        raise ValueError("unsupported split")
    lo_rows = rows // 2
    half_cols = cols // 2
    full = n <= 8 and n & (n - 1) == 0

    place = lax.axis_index("gz")
    limits = jnp.broadcast_to(thresholds[:, None, None], (count, 8, half_cols))
    where = place.astype(jnp.int32)[None]

    other = shifted(noisy_cube, "gy", 1)
    across, y_matrix, cube = call(
        first_kernel,
        (
            struct(cols, cols), struct(rows, 2 * rows), struct(planes, rows, cols),
        ), 0, [pl.BlockSpec(memory_space=pltpu.HBM)], [pltpu.SemaphoreType.DMA],
    )(noisy_cube)
    flat, far = call(
        plane_kernel, (struct(planes, rows, cols), struct(2, rows, cols)), 1, [VMEM] * 4,
        [scratch(planes * rows, cols)],
    )(where, cube, other, y_matrix, across)

    level = exchanged(flat, lambda i: i + 2 if i % 2 else i - 2)
    mate = exchanged(flat, lambda i: i ^ 1)
    far = exchanged(far, lambda i: i - 2 if i % 2 else i + 2)
    half = functools.partial(jax.ShapeDtypeStruct, dtype=jnp.bfloat16)
    block = planes * rows
    x_matrix, deep_across, both_x, back_y, both_y = call(
        second_kernel,
        (
            struct(cols, cols), struct(half_cols, half_cols), half((2, half_cols, cols)),
            struct(rows, rows + EDGE), half((2, block, block)),
        ), 0, [], [scratch(half_cols, half_cols), scratch(block, block)],
    )()
    parcel = call(
        depth_kernel, struct(planes // 2 * lo_rows + 2 * count, half_cols), 1, [VMEM] * 5,
        [scratch(planes // 2 * lo_rows, half_cols)],
    )(where, limits, flat, mate, level, deep_across)

    if full:
        pairs = n // 2
        column = jnp.stack([parcel, exchanged(parcel, lambda i: i ^ 1)])
        side = [column]
        for q in range(1, pairs):
            side.append(exchanged(column, lambda i: i ^ 2 * q))
        side = jnp.concatenate(side)
    else:
        side = jnp.stack([parcel if o == 0 else shifted(parcel, "gz", -o) for o in range(-5, 6)])
    parcels = jnp.stack([side, shifted(side, "gy", 1)])

    cross = exchanged(level, lambda i: i ^ 1)
    coefs, edge = call(
        stack_kernel, (struct(10, rows, cols), struct(10, EDGE, cols)), 1, [VMEM] * 5
    )(where, flat, mate, level, cross, far)
    edge = shifted(edge, "gy", 1)
    detail = call(
        detail_kernel, struct(count, planes, rows, cols), 0, [VMEM] * 5,
        [scratch(count * planes, rows + EDGE, cols), scratch(count * planes * rows, cols)],
        flops=20_000_000,
    )(limits, coefs, edge, back_y, x_matrix)

    kappas = n if full else 6
    cells = float(planes * rows * cols * n * 2)
    denoised, score = call(
        functools.partial(final_kernel, full, cells),
        (struct(planes, count, rows, cols), struct(count if full else 2 * count)), 1, [VMEM] * 5,
        [
            scratch(2 * kappas, rows + EDGE, half_cols),
            scratch(2 * kappas * rows, half_cols),
            scratch(count * block, half_cols),
            scratch(count, planes, rows, cols),
            pltpu.SMEM((count if full else 2 * count,), jnp.float32),
            pltpu.SemaphoreType.DMA((count + 1,)),
        ],
        score=True,
    )(where, limits, parcels, detail, both_y, both_x)
    if not full:
        total = lax.psum(score, ("gz", "gy"))
        score = cells * total[count:] / (total[:count] * total[:count])
    return denoised, score


def solution(mesh):
    in_specs = (P(("cube", "gz"), "gy", None), P())
    out_specs = (P(("cube", "gz"), None, "gy", None), P("cube"))
    return jax.shard_map(body, mesh=mesh, in_specs=in_specs, out_specs=out_specs, check_vma=False)
```

```python
import functools
import jax
import jax.numpy as jnp
from jax import lax
from jax.experimental import pallas as pl
from jax.experimental.pallas import tpu as pltpu
from jax.sharding import PartitionSpec as P


LOWPASS = (
    0.2303778133088964,
    0.7148465705529155,
    0.6308807679298587,
    -0.0279837694168599,
    -0.1870348117190931,
    0.0308413818355607,
    0.0328830116668852,
    -0.010597401785069,
)
HIGHPASS = tuple((-1) ** tap * LOWPASS[7 - tap] for tap in range(8))
FILTERS = (LOWPASS, HIGHPASS)
EDGE = 8


def dot(a, b, contract=0):
    return lax.dot_general(
        a, b, (((1,), (contract,)), ((), ())),
        precision=lax.Precision.HIGHEST, preferred_element_type=jnp.float32,
    )


def weighted(terms):
    total = None
    for weight, value in terms:
        part = value * weight
        total = part if total is None else total + part
    return total


def filter_tile(first, position, length, band):
    gap = position - first
    gap = jnp.where(gap < 0, gap + length, gap)
    value = jnp.zeros(gap.shape, jnp.float32)
    for tap in range(8):
        value = jnp.where(gap == tap, FILTERS[band][tap], value)
    return value


def iota(shape, dimension):
    return lax.broadcasted_iota(jnp.int32, shape, dimension)


def edge_rows(row, last):
    return last - 2 + row % 4


def analysis_tiles(ref, across=False):
    length = ref.shape[0]
    half = length // 2
    for band in range(2):
        shape = (length, half) if across else (half, length)
        value = filter_tile(2 * iota(shape, int(across)), iota(shape, 1 - int(across)), length, band)
        if across:
            ref[:, pl.ds(band * half, half)] = value
        else:
            ref[pl.ds(band * half, half), :] = value


def split(value):
    high = value.astype(jnp.bfloat16)
    return high, (value - high.astype(jnp.float32)).astype(jnp.bfloat16)


def split_dot(a, b):
    def part(left, right):
        return lax.dot_general(left, right, (((1,), (0,)), ((), ())), preferred_element_type=jnp.float32)

    return part(a[0], b[0]) + (part(a[0], b[1]) + part(a[1], b[0]))


def blocks(shape, block):
    row, column = iota(shape, 0), iota(shape, 1)
    return row % block, column % block, row // block == column // block


def first_kernel(cube_ref, across_ref, y_ref, cube_out_ref, semaphore):
    copy = pltpu.make_async_copy(cube_ref, cube_out_ref, semaphore)
    copy.start()
    rows, length = y_ref.shape
    half = rows // 2
    for band in range(2):
        shape = (half, length)
        y_ref[pl.ds(band * half, half), :] = filter_tile(2 * iota(shape, 0), iota(shape, 1), length, band)
    analysis_tiles(across_ref, True)
    copy.wait()


def second_kernel(x_ref, deep_across_ref, both_x_ref, back_y_ref, both_y_ref, deep_x, deep_y):
    analysis_tiles(x_ref)
    analysis_tiles(deep_across_ref, True)
    analysis_tiles(deep_x)
    half_cols = deep_x.shape[0]
    both_x_ref[0], both_x_ref[1] = split(dot(deep_x[...], x_ref[pl.ds(0, half_cols), :]))
    shape = back_y_ref.shape
    rows = shape[0]
    half = rows // 2
    sample, column = iota(shape, 0), iota(shape, 1)
    total = jnp.zeros(shape, jnp.float32)
    for band in range(2):
        value = filter_tile(2 * (column - band * half), sample, 2 * rows, band)
        total = jnp.where((column >= band * half) & (column < (band + 1) * half), value, total)
        start = rows + band * 4
        value = filter_tile(2 * edge_rows(column - start, -1), sample, 2 * rows, band)
        total = jnp.where((column >= start) & (column < start + 3), value, total)
    back_y_ref[...] = total
    row, column, mask = blocks(deep_y.shape, rows)
    first = 2 * jnp.where(row < half, row, row - half)
    lo = filter_tile(first, column, rows, 0)
    hi = filter_tile(first, column, rows, 1)
    deep_y[...] = jnp.where(mask, jnp.where(row < half, lo, hi), 0.0)
    lows = jnp.where(mask, filter_tile(2 * column, row, 2 * rows, 0), 0.0)
    both_y_ref[0], both_y_ref[1] = split(dot(lows, deep_y[...], 1))


def plane_kernel(place_ref, own_ref, other_ref, y_ref, x_ref, out_ref, far_ref, mid):
    planes, rows, _ = own_ref.shape
    for z in range(planes):
        plane = jnp.concatenate([own_ref[z], other_ref[z]], 0)
        mid[pl.ds(z * rows, rows), :] = dot(y_ref[...], plane)
    result = dot(mid[...], x_ref[...])
    odd = place_ref[0] % 2 == 1
    for z in range(planes):
        out_ref[z] = result[z * rows : (z + 1) * rows]
    for z in range(2):
        head = result[z * rows : (z + 1) * rows]
        tail = result[(planes - 2 + z) * rows : (planes - 1 + z) * rows]
        far_ref[z] = jnp.where(odd, head, tail)


def tally(values, limit_squares, sums, keep=None):
    parts = [value * value for value in values]
    for t, limit in enumerate(limit_squares):
        bases = [part + limit for part in parts]
        cuts = [jnp.minimum(part, limit) for part in parts]
        tops = [1.0] * len(bases)
        while len(bases) > 1:
            tops = [tops[i] * bases[i + 1] + tops[i + 1] * bases[i] for i in range(0, len(bases), 2)]
            bases = [bases[i] * bases[i + 1] for i in range(0, len(bases), 2)]
        weight = tops[0] / bases[0]
        cut = functools.reduce(jnp.add, cuts)
        if keep is not None:
            weight = jnp.where(keep, weight, 0.0)
            cut = jnp.where(keep, cut, 0.0)
        sums[0][t] = weight if sums[0][t] is None else sums[0][t] + weight
        sums[1][t] = cut if sums[1][t] is None else sums[1][t] + cut


def fold(sums):
    rows = [jnp.sum(a, axis=0, keepdims=True) for group in sums for a in group]
    return jnp.concatenate(rows, 0)


def depth_kernel(place_ref, limits_ref, own_ref, mate_ref, level_ref, deep_across_ref, parcel_ref, lows):
    planes, rows, cols = own_ref.shape
    count = limits_ref.shape[0]
    squares = [limits_ref[t] * limits_ref[t] for t in range(count)]
    half_cols = cols // 2
    lo_rows = rows // 2
    odd = place_ref[0] % 2 == 1
    sums = [[None] * count, [None] * count]
    for r in range(0, rows, 8):
        for c in range(0, cols, half_cols):
            at = (pl.ds(r, 8), pl.ds(c, half_cols))
            own = [own_ref[(i,) + at] for i in range(planes)]
            level = [level_ref[(i,) + at] for i in range(planes)]
            tile = [jnp.where(odd, level[i], own[i]) for i in range(planes)]
            tile += [mate_ref[(i,) + at] for i in range(planes)]
            tile += [jnp.where(odd, own[i], level[i]) for i in range(2)]
            counted = []
            for k in range(planes // 2):
                for band in range(2):
                    value = weighted((FILTERS[band][tap], tile[2 * k + tap]) for tap in range(8))
                    if band == 0 and c == 0 and r < lo_rows:
                        lows[pl.ds(k * lo_rows + r, 8), :] = value
                    else:
                        counted.append(value)
            tally(counted, squares, sums)
    parcel_ref[pl.ds(0, planes // 2 * lo_rows), :] = dot(lows[...], deep_across_ref[...])
    parcel_ref[pl.ds(planes // 2 * lo_rows, 2 * count), :] = fold(sums)


def stack_kernel(place_ref, own_ref, mate_ref, level_ref, cross_ref, far_ref, out_ref, edge_ref):
    planes, rows, cols = own_ref.shape
    half_cols = cols // 2
    odd = place_ref[0] % 2 == 1
    for r in range(0, rows, 8):
        for c in range(0, cols, half_cols):
            at = (pl.ds(r, 8), pl.ds(c, half_cols))
            mate = [mate_ref[(i,) + at] for i in range(planes)]
            cross = [cross_ref[(i,) + at] for i in range(planes)]
            level = [level_ref[(i,) + at] for i in range(planes)]
            far = [far_ref[(i,) + at] for i in range(2)]
            tile = [jnp.where(odd, level[planes - 2 + i], far[i]) for i in range(2)]
            tile += [jnp.where(odd, mate[i], cross[i]) for i in range(planes)]
            tile += [own_ref[(i,) + at] for i in range(planes)]
            tile += [jnp.where(odd, cross[i], mate[i]) for i in range(planes)]
            tile += [jnp.where(odd, far[i], level[i]) for i in range(2)]
            for k in range(5):
                for band in range(2):
                    value = weighted((FILTERS[band][tap], tile[2 * k + tap]) for tap in range(8))
                    out_ref[(2 * k + band,) + at] = value
    edge_ref[...] = jnp.zeros(edge_ref.shape, jnp.float32)
    for k in range(10):
        for band in range(2):
            stop = (band + 1) * rows // 2
            edge_ref[k, pl.ds(band * 4, 3), :] = out_ref[k, pl.ds(stop - 3, 3), :]


def detail_kernel(limits_ref, coefs_ref, edge_ref, back_y_ref, x_ref, out_ref, wide, wide_y):
    count, planes = out_ref.shape[0], out_ref.shape[1]
    _, rows, cols = coefs_ref.shape
    half_cols = cols // 2
    lo_rows = rows // 2
    limits = [limits_ref[t] for t in range(count)]
    low_edge = iota((8, half_cols), 0) < 4
    for r in range(0, rows + EDGE, 8):
        for c in range(0, cols, half_cols):
            if r < rows:
                tile = [coefs_ref[i, pl.ds(r, 8), pl.ds(c, half_cols)] for i in range(10)]
            else:
                tile = [edge_ref[i, :, pl.ds(c, half_cols)] for i in range(10)]
            for t in range(count):
                shrunk = {}
                for i, value in enumerate(tile):
                    kap, band = i // 2 - 3, i % 2
                    if band == 0 and c == 0 and r < lo_rows:
                        continue
                    cut = value - jnp.clip(value, -limits[t], limits[t])
                    if band == 0 and c == 0 and r >= rows:
                        cut = jnp.where(low_edge, 0.0, cut)
                    shrunk[kap, band] = cut
                for z in range(planes):
                    wide[t * planes + z, pl.ds(r, 8), pl.ds(c, half_cols)] = weighted(
                        (FILTERS[band][2 * j + z % 2], shrunk[z // 2 - j, band])
                        for j in range(4) for band in range(2) if (z // 2 - j, band) in shrunk
                    )
    for s in range(count * planes):
        wide_y[pl.ds(s * rows, rows), :] = dot(back_y_ref[...], wide[s])
    result = dot(wide_y[...], x_ref[...])
    for t in range(count):
        for z in range(planes):
            s = t * planes + z
            out_ref[t, z] = result[s * rows : (s + 1) * rows]


def way_back(z):
    weights = {}
    for i in range(4):
        plane = z // 2 - i
        for j in range(4):
            for band in range(2):
                at = (plane // 2 - j, band)
                weights[at] = weights.get(at, 0.0) + LOWPASS[2 * i + z % 2] * FILTERS[band][2 * j + plane % 2]
    return weights


def final_kernel(
    full, cells, place_ref, limits_ref, parcels_ref, detail_ref, both_y_ref, both_x_ref,
    out_ref, score_ref, zed, mix, coarse, staged, scores, semaphores,
):
    count, planes, rows, cols = detail_ref.shape
    half_cols = cols // 2
    limits = [limits_ref[t] for t in range(count)]
    squares = [t * t for t in limits]
    depth = planes // 2
    lo_rows = (parcels_ref.shape[2] - 2 * count) // depth
    deep_rows = 2 * lo_rows
    pieces = parcels_ref.shape[1]
    kappas = list(range(-5, -5 + pieces)) if full else list(range(-5, 1))
    here = place_ref[0]

    def piece(spot):
        spot = here + 2 * pieces + spot
        if not full:
            return spot + 2 * (spot % 2) - here - 2 * pieces + 5
        owner = (spot + 2 * (spot % 2)) % pieces
        return ((owner // 2) ^ (here // 2)) * 2 + ((owner % 2) ^ (here % 2))

    def reach(kap, tap):
        r = 2 * kap + 10 + tap
        return r % (depth * pieces) if full else r

    used = sorted({reach(kap, tap) for kap in kappas for tap in range(8)})
    spots = {r // depth: piece(r // depth - 5) for r in used}
    for side in range(2):
        for i in range(0, lo_rows, 8):
            tile = {r: parcels_ref[side, spots[r // depth], pl.ds((r % depth) * lo_rows + i, 8), :] for r in used}
            for a, kap in enumerate(kappas):
                for band in range(2):
                    value = weighted((FILTERS[band][tap], tile[reach(kap, tap)]) for tap in range(8))
                    zed[2 * a + band, pl.ds(side * lo_rows + i, 8), :] = value
                    if side == 0 and i == 0:
                        zed[2 * a + band, pl.ds(deep_rows, 8), :] = value
    for a in range(2 * len(kappas)):
        for i in range(0, lo_rows, 8):
            tile = [zed[a, pl.ds(2 * i + tap, 8, stride=2), :] for tap in range(8)]
            for band in range(2):
                mix[pl.ds(a * deep_rows + band * lo_rows + i, 8), :] = weighted(zip(FILTERS[band], tile))

    low_lanes = iota((8, half_cols), 1) < half_cols // 2
    block = planes * rows
    both_y = (both_y_ref[0], both_y_ref[1])
    both_x = (both_x_ref[0], both_x_ref[1])
    copies = []
    for t in range(count):
        if t == count - 1:
            sums = [[None] * count, [None] * count]
            for a, kap in enumerate(kappas):
                if not full and kap != 0:
                    continue
                counted = []
                for band in range(2):
                    for i in range(0, deep_rows, 8):
                        if not full and i % lo_rows >= lo_rows // 2:
                            continue
                        value = mix[pl.ds((2 * a + band) * deep_rows + i, 8), :]
                        if band == 0 and i < lo_rows:
                            tally([value], squares, sums, ~low_lanes)
                        else:
                            counted.append(value)
                for i in range(0, len(counted), 2):
                    tally(counted[i : i + 2], squares, sums)
            total = fold(sums)
            if full:
                for side in range(2):
                    for at in range(pieces):
                        total = total + parcels_ref[side, at, pl.ds(depth * lo_rows, 2 * count), :]
            else:
                total = total + parcels_ref[0, 5, pl.ds(depth * lo_rows, 2 * count), :]
            for u in range(count):
                weight = jnp.sum(total[u : u + 1] * squares[u][:1])
                residual = jnp.sum(total[count + u : count + u + 1])
                if full:
                    scores[u] = cells * residual / (weight * weight)
                else:
                    scores[u] = weight
                    scores[count + u] = residual
            copies.append(pltpu.make_async_copy(scores, score_ref, semaphores.at[count]))
            copies[-1].start()
        for i in range(0, deep_rows, 8):
            shrunk = {}
            for a, kap in enumerate(kappas):
                if kap > 0:
                    continue
                for band in range(2):
                    value = mix[pl.ds((2 * a + band) * deep_rows + i, 8), :]
                    cut = value - jnp.clip(value, -limits[t], limits[t])
                    if band == 0 and i < lo_rows:
                        cut = jnp.where(low_lanes, value, cut)
                    shrunk[kap, band] = cut
            for z in range(planes):
                coarse[pl.ds((t * planes + z) * rows + i, 8), :] = weighted(
                    (weight, shrunk[at]) for at, weight in way_back(z).items()
                )
        result = split_dot(both_y, split(coarse[pl.ds(t * block, block), :]))
        result = split_dot(split(result), both_x)
        for z in range(planes):
            staged[t, z] = detail_ref[t, z] + result[z * rows : (z + 1) * rows]
        copies.append(pltpu.make_async_copy(staged.at[t], out_ref.at[:, t], semaphores.at[t]))
        copies[-1].start()

    for copy in copies:
        copy.wait()


def shifted(array, axis, by):
    devices = lax.axis_size(axis)
    return lax.ppermute(array, axis, [(i, (i + by) % devices) for i in range(devices)])


def exchanged(array, partner):
    devices = lax.axis_size("gz")
    return lax.ppermute(array, "gz", [(i, partner(i) % devices) for i in range(devices)])


VMEM = pl.BlockSpec(memory_space=pltpu.VMEM)
SMEM = pl.BlockSpec(memory_space=pltpu.SMEM)
PARAMS = pltpu.CompilerParams(vmem_limit_bytes=24 * 1024 * 1024)


def struct(*shape):
    return jax.ShapeDtypeStruct(shape, jnp.float32)


def scratch(*shape):
    return pltpu.VMEM(shape, jnp.float32)


def call(kernel, out_shape, smem, vmem, scratches=(), score=False, flops=100_000):
    out_specs = jax.tree.map(lambda _: VMEM, out_shape)
    if score:
        out_specs = (pl.BlockSpec(memory_space=pltpu.HBM),) * 2

    def run(*operands):
        return pl.pallas_call(
            kernel,
            out_shape=out_shape,
            in_specs=[SMEM] * smem + vmem,
            out_specs=out_specs,
            scratch_shapes=list(scratches),
            compiler_params=PARAMS,
            cost_estimate=pl.CostEstimate(flops=flops, bytes_accessed=0, transcendentals=0),
        )(*operands)

    return run


def body(noisy_cube, thresholds):
    planes, rows, cols = noisy_cube.shape
    count = thresholds.shape[0]
    n = lax.axis_size("gz")
    if lax.axis_size("gy") != 2 or planes != 4 or n % 4:
        raise ValueError("unsupported split")
    lo_rows = rows // 2
    half_cols = cols // 2
    full = n <= 8 and n & (n - 1) == 0

    place = lax.axis_index("gz")
    limits = jnp.broadcast_to(thresholds[:, None, None], (count, 8, half_cols))
    where = place.astype(jnp.int32)[None]

    other = shifted(noisy_cube, "gy", 1)
    across, y_matrix, cube = call(
        first_kernel,
        (
            struct(cols, cols), struct(rows, 2 * rows), struct(planes, rows, cols),
        ), 0, [pl.BlockSpec(memory_space=pltpu.HBM)], [pltpu.SemaphoreType.DMA],
    )(pltpu.with_memory_space_constraint(noisy_cube, pltpu.HBM))
    flat, far = call(
        plane_kernel, (struct(planes, rows, cols), struct(2, rows, cols)), 1, [VMEM] * 4,
        [scratch(planes * rows, cols)],
    )(where, cube, other, y_matrix, across)

    level = exchanged(flat, lambda i: i + 2 if i % 2 else i - 2)
    mate = exchanged(flat, lambda i: i ^ 1)
    far = exchanged(far, lambda i: i - 2 if i % 2 else i + 2)
    half = functools.partial(jax.ShapeDtypeStruct, dtype=jnp.bfloat16)
    block = planes * rows
    x_matrix, deep_across, both_x, back_y, both_y = call(
        second_kernel,
        (
            struct(cols, cols), struct(half_cols, half_cols), half((2, half_cols, cols)),
            struct(rows, rows + EDGE), half((2, block, block)),
        ), 0, [], [scratch(half_cols, half_cols), scratch(block, block)],
    )()
    parcel = call(
        depth_kernel, struct(planes // 2 * lo_rows + 2 * count, half_cols), 1, [VMEM] * 5,
        [scratch(planes // 2 * lo_rows, half_cols)],
    )(where, limits, flat, mate, level, deep_across)

    if full:
        pairs = n // 2
        column = jnp.stack([parcel, exchanged(parcel, lambda i: i ^ 1)])
        side = [column]
        for q in range(1, pairs):
            side.append(exchanged(column, lambda i: i ^ 2 * q))
        side = jnp.concatenate(side)
    else:
        side = jnp.stack([parcel if o == 0 else shifted(parcel, "gz", -o) for o in range(-5, 6)])
    parcels = jnp.stack([side, shifted(side, "gy", 1)])

    cross = exchanged(level, lambda i: i ^ 1)
    coefs, edge = call(
        stack_kernel, (struct(10, rows, cols), struct(10, EDGE, cols)), 1, [VMEM] * 5
    )(where, flat, mate, level, cross, far)
    edge = shifted(edge, "gy", 1)
    detail = call(
        detail_kernel, struct(count, planes, rows, cols), 0, [VMEM] * 5,
        [scratch(count * planes, rows + EDGE, cols), scratch(count * planes * rows, cols)],
        flops=20_000_000,
    )(limits, coefs, edge, back_y, x_matrix)

    kappas = n if full else 6
    cells = float(planes * rows * cols * n * 2)
    denoised, score = call(
        functools.partial(final_kernel, full, cells),
        (struct(planes, count, rows, cols), struct(count if full else 2 * count)), 1, [VMEM] * 5,
        [
            scratch(2 * kappas, rows + EDGE, half_cols),
            scratch(2 * kappas * rows, half_cols),
            scratch(count * block, half_cols),
            scratch(count, planes, rows, cols),
            pltpu.SMEM((count if full else 2 * count,), jnp.float32),
            pltpu.SemaphoreType.DMA((count + 1,)),
        ],
        score=True,
    )(where, limits, parcels, detail, both_y, both_x)
    if not full:
        total = lax.psum(score, ("gz", "gy"))
        score = cells * total[count:] / (total[:count] * total[:count])
    return denoised, score


def solution(mesh):
    in_specs = (P(("cube", "gz"), "gy", None), P())
    out_specs = (P(("cube", "gz"), None, "gy", None), P("cube"))
    return jax.shard_map(body, mesh=mesh, in_specs=in_specs, out_specs=out_specs, check_vma=False)
```
